16 devices in a mesh: dp: 2 (over y, z), ep: 8 (over x, core).
Axes of the slice: x: 4, y: 2, z: 1, core: 2. Of those that a mesh axis runs over, the one named last changes fastest.
The devices are a block of a 4x4x8 slice.
Arguments:
- x: bfloat16 [48, 64, 2048], P(('dp', 'ep')), parts along dimension 0
- idx: int32 [48, 64, 8], P(('dp', 'ep')), parts along dimension 0
- gates: float32 [48, 64, 8], P(('dp', 'ep')), parts along dimension 0
- g1: float32 [2048], replicated
- wq: bfloat16 [2048, 2048], replicated
- wk: bfloat16 [2048, 2048], replicated
- wv: bfloat16 [2048, 2048], replicated
- wo: bfloat16 [2048, 2048], replicated
- g2: float32 [2048], replicated
- w1: bfloat16 [64, 2048, 1024], P('ep')
- w3: bfloat16 [64, 2048, 1024], P('ep')
- w2: bfloat16 [64, 1024, 2048], P('ep')
Outputs:
- output: bfloat16 [48, 64, 2048], P(('dp', 'ep')), parts along dimension 0
There are 2 independent parts. The reference program is written for one: setup_inputs(seed, part) draws one part's arguments, and reference() takes and returns one part's arrays. A program takes and returns all parts, laid end to end along the dimension named above; an argument that names none is the same for every part.
All inputs are finite; a program needn't handle non-finite values.
Results may differ from the reference program's by a relative error of at most 0.0112406.
Values are sent between devices in bfloat16 or wider.
A program may use at most 768 MiB of HBM per device.

```python
import jax
import jax.numpy as jnp
from jax import lax

D = 2048
HEADS = 16
HEAD = 128
EXPERTS = 64
TOP = 8
FF = 1024
SEQ = 64
SEQS = 3
EP = 8

TOK = SEQS * SEQ
AVG = TOP * TOK // EXPERTS
CAP = AVG + AVG // 2
EPS = 1e-6


def draw_routes(kk, shift):
    k1, k2, k3, k4 = jax.random.split(kk, 4)
    signs = jnp.roll(jnp.where(jnp.arange(EXPERTS) < EXPERTS // 2, 1, -1), shift)
    counts = AVG + (AVG // 2) * signs
    ends = jnp.cumsum(counts)
    ent = jnp.searchsorted(ends, jnp.arange(TOP * TOK), side='right').astype(jnp.int32)
    grid = ent.reshape(TOP, TOK).T
    grid = jnp.roll(grid, jax.random.randint(k2, (), 0, TOK), axis=0)
    gates = 2.5 * jax.nn.softmax(0.5 * jax.random.normal(k4, (TOK, TOP), jnp.float32), axis=-1)
    return grid, gates


def setup_inputs(seed: int = 0, part: int = 0) -> dict:
    kp = jax.random.fold_in(jax.random.key(seed), part)
    kx, kr = jax.random.split(kp)
    x = jax.random.normal(kx, (EP * SEQS, SEQ, D), jnp.float32).astype(jnp.bfloat16)
    shift = jax.random.randint(jax.random.fold_in(kr, 7), (), 0, EXPERTS)
    idx, gates = jax.vmap(lambda kk: draw_routes(kk, shift))(jax.random.split(kr, EP))
    ks = jax.random.split(jax.random.key(seed + 1), 9)
    wid = HEADS * HEAD

    def mat(k, shape, scale):
        return (scale * jax.random.normal(k, shape, jnp.float32)).astype(jnp.bfloat16)

    return {
        'x': x,
        'idx': idx.reshape(EP * SEQS, SEQ, TOP),
        'gates': gates.reshape(EP * SEQS, SEQ, TOP),
        'g1': jax.random.uniform(ks[0], (D,), jnp.float32, 0.5, 1.5),
        'wq': mat(ks[1], (D, wid), 1.4 * D ** -0.5),
        'wk': mat(ks[2], (D, wid), 1.4 * D ** -0.5),
        'wv': mat(ks[3], (D, wid), D ** -0.5),
        'wo': mat(ks[4], (wid, D), 2.0 * wid ** -0.5),
        'g2': jax.random.uniform(ks[5], (D,), jnp.float32, 0.5, 1.5),
        'w1': mat(ks[6], (EXPERTS, D, FF), D ** -0.5),
        'w3': mat(ks[7], (EXPERTS, D, FF), D ** -0.5),
        'w2': mat(ks[8], (EXPERTS, FF, D), FF ** -0.5),
    }


def rms(x, g):
    xf = x.astype(jnp.float32)
    return (xf * lax.rsqrt(jnp.mean(xf * xf, axis=-1, keepdims=True) + EPS) * g).astype(jnp.bfloat16)


def attend(q, k, v):
    n = q.shape[0]
    s = jnp.einsum('qhd,khd->hqk', q.astype(jnp.float32), k.astype(jnp.float32)) * HEAD ** -0.5
    mask = jnp.arange(n)[:, None] >= jnp.arange(n)[None, :]
    s = jnp.where(mask[None], s, -1e30)
    p = jax.nn.softmax(s, axis=-1).astype(jnp.bfloat16)
    o = jnp.einsum('hqk,khd->qhd', p.astype(jnp.float32), v.astype(jnp.float32))
    return o.astype(jnp.bfloat16)


def slot_pos(flat):
    n = flat.shape[0]
    order = jnp.argsort(flat, stable=True)
    se = flat[order]
    counts = jnp.zeros((EXPERTS,), jnp.int32).at[flat].add(1)
    starts = jnp.cumsum(counts) - counts
    ps = jnp.arange(n, dtype=jnp.int32) - starts[se]
    return jnp.zeros((n,), jnp.int32).at[order].set(ps)


def expert(a):
    r, a1, a3, a2 = a
    h1 = jnp.dot(r, a1, preferred_element_type=jnp.float32)
    h3 = jnp.dot(r, a3, preferred_element_type=jnp.float32)
    u = (jax.nn.silu(h1) * h3).astype(jnp.bfloat16)
    return jnp.dot(u, a2, preferred_element_type=jnp.float32).astype(jnp.bfloat16)


def reference(x, idx, gates, g1, wq, wk, wv, wo, g2, w1, w3, w2):
    n, s_len, d = x.shape
    t_all = n * s_len
    xf = x.reshape(t_all, d)
    xn = rms(xf, g1)

    def proj(w):
        return jnp.dot(xn, w, preferred_element_type=jnp.float32).astype(jnp.bfloat16).reshape(n, s_len, HEADS, HEAD)

    q = proj(wq)
    k = proj(wk)
    v = proj(wv)
    o = lax.map(lambda a: attend(a[0], a[1], a[2]), (q, k, v))
    att = jnp.dot(o.reshape(t_all, HEADS * HEAD), wo, preferred_element_type=jnp.float32).astype(jnp.bfloat16)
    h = (xf.astype(jnp.float32) + att.astype(jnp.float32)).astype(jnp.bfloat16)
    z = rms(h, g2)
    zs = z.reshape(EP, TOK, d)
    flat = idx.reshape(EP, TOK * TOP)
    dest = flat * CAP + jax.vmap(slot_pos)(flat)
    rows = jnp.repeat(zs, TOP, axis=1)
    buf = jax.vmap(lambda dd, rr: jnp.zeros((EXPERTS * CAP, d), jnp.bfloat16).at[dd].set(rr))(dest, rows)
    buf = buf.reshape(EP, EXPERTS, CAP, d).transpose(1, 0, 2, 3).reshape(EXPERTS, EP * CAP, d)
    out = lax.map(expert, (buf, w1, w3, w2))
    out = out.reshape(EXPERTS, EP, CAP, d).transpose(1, 0, 2, 3).reshape(EP, EXPERTS * CAP, d)
    got = jax.vmap(lambda oo, dd: oo[dd])(out, dest)
    got = got.reshape(t_all, TOP, d).astype(jnp.float32)
    moe = jnp.sum(got * gates.reshape(t_all, TOP, 1), axis=1)
    y = (h.astype(jnp.float32) + moe).astype(jnp.bfloat16)
    return y.reshape(n, s_len, d)
```

```python
import functools

import jax
import jax.numpy as jnp
from jax import lax
from jax.experimental import pallas as pl
from jax.experimental.pallas import tpu as pltpu
from jax.sharding import PartitionSpec as P

EPS = 1e-6
HEAD = 128
F32, BF16 = jnp.float32, jnp.bfloat16


def rms(xf, g):
    return (xf * lax.rsqrt(jnp.mean(xf * xf, axis=-1, keepdims=True) + EPS) * g).astype(BF16)


def attn_kernel(hb, seq, x_ref, g1_ref, g2_ref, wq_ref, wk_ref, wv_ref, wo_ref, h_ref, z_ref, xn_ref, acc_ref):
    i = pl.program_id(0)
    t = x_ref.shape[0]

    @pl.when(i == 0)
    def _():
        xn_ref[...] = rms(x_ref[...].astype(F32), g1_ref[...])
        acc_ref[...] = jnp.zeros_like(acc_ref)

    xn = xn_ref[...]
    q = jnp.dot(xn, wq_ref[...], preferred_element_type=F32).astype(BF16)
    k = jnp.dot(xn, wk_ref[...], preferred_element_type=F32).astype(BF16)
    v = jnp.dot(xn, wv_ref[...], preferred_element_type=F32).astype(BF16)
    row = lax.broadcasted_iota(jnp.int32, (t, t), 0)
    col = lax.broadcasted_iota(jnp.int32, (t, t), 1)
    mask = (row >= col) & (row // seq == col // seq)
    outs = []
    for j in range(hb):
        sl = slice(j * HEAD, (j + 1) * HEAD)
        s = lax.dot_general(q[:, sl], k[:, sl], (((1,), (1,)), ((), ())), preferred_element_type=F32) * HEAD ** -0.5
        s = jnp.where(mask, s, -1e30)
        e = jnp.exp(s - jnp.max(s, axis=-1, keepdims=True))
        p = (e / jnp.sum(e, axis=-1, keepdims=True)).astype(BF16)
        outs.append(jnp.dot(p, v[:, sl], preferred_element_type=F32).astype(BF16))
    o = jnp.concatenate(outs, axis=1)
    acc_ref[...] += jnp.dot(o, wo_ref[...], preferred_element_type=F32)

    @pl.when(i == pl.num_programs(0) - 1)
    def _():
        att = acc_ref[...].astype(BF16)
        h = (x_ref[...].astype(F32) + att.astype(F32)).astype(BF16)
        h_ref[...] = h
        z_ref[...] = rms(h.astype(F32), g2_ref[...])


def attention(xf, g1, g2, wq, wk, wv, wo, seq, hb=2):
    t, d = xf.shape
    wid = wq.shape[1]
    c = hb * HEAD
    return pl.pallas_call(
        functools.partial(attn_kernel, hb, seq),
        grid=(wid // c,),
        in_specs=[
            pl.BlockSpec((t, d), lambda i: (0, 0)),
            pl.BlockSpec((1, d), lambda i: (0, 0)),
            pl.BlockSpec((1, d), lambda i: (0, 0)),
            pl.BlockSpec((d, c), lambda i: (0, i)),
            pl.BlockSpec((d, c), lambda i: (0, i)),
            pl.BlockSpec((d, c), lambda i: (0, i)),
            pl.BlockSpec((c, d), lambda i: (i, 0)),
        ],
        out_specs=[pl.BlockSpec((t, d), lambda i: (0, 0))] * 2,
        out_shape=[jax.ShapeDtypeStruct((t, d), BF16)] * 2,
        scratch_shapes=[pltpu.VMEM((t, d), BF16), pltpu.VMEM((t, d), F32)],
        compiler_params=pltpu.CompilerParams(dimension_semantics=("arbitrary",), vmem_limit_bytes=48 * 2**20),
        cost_estimate=pl.CostEstimate(flops=8 * t * d * wid, bytes_accessed=8 * d * wid, transcendentals=0),
        name="attention",
    )(xf, g1.reshape(1, d), g2.reshape(1, d), wq, wk, wv, wo)


def split3(g):
    hi = lax.reduce_precision(g, 8, 7)
    mid = lax.reduce_precision(g - hi, 8, 7)
    return hi, mid, g - hi - mid


def solution(mesh):
    ep = mesh.shape['ep']
    tok = P(('dp', 'ep'))
    rep = P()
    exs = P('ep')

    def body(x, idx, gates, g1, wq, wk, wv, wo, g2, w1, w3, w2):
        n, s_len, d = x.shape
        t = n * s_len
        top = idx.shape[-1]
        g_loc = w1.shape[0]
        avg = top * t // (g_loc * ep)
        cap = avg + avg // 2
        h, z = attention(x.reshape(t, d), g1, g2, wq, wk, wv, wo, s_len)

        meta = jnp.concatenate([idx.reshape(t, top).astype(F32), gates.reshape(t, top)], axis=1)
        meta = lax.all_gather(meta, 'ep')
        ids, gt = meta[..., :top], meta[..., top:]
        mine = (lax.axis_index('ep') * g_loc + jnp.arange(g_loc)).astype(F32)
        hit = ids[:, :, :, None] == mine
        mask = jnp.any(hit, axis=2)
        gate = jnp.sum(jnp.where(hit, gt[:, :, :, None], 0.0), axis=2)
        tri = (jnp.arange(t)[:, None] > jnp.arange(t)[None, :]).astype(BF16)
        rank = jnp.einsum('ut,ste->sue', tri, mask.astype(BF16), preferred_element_type=F32)
        place = jnp.where(mask, rank, -1.0)
        sel = place[..., None] == jnp.arange(cap, dtype=F32)
        sel = sel.reshape(ep, t, g_loc * cap)
        gate = jnp.broadcast_to(gate[..., None], gate.shape + (cap,)).reshape(sel.shape)
        zs = lax.all_gather(z, 'ep')
        r = jnp.einsum('str,std->srd', sel.astype(BF16), zs, preferred_element_type=F32).astype(BF16)
        r = r.reshape(ep, g_loc, cap, d).transpose(1, 0, 2, 3).reshape(g_loc, ep * cap, d)
        h1 = jnp.einsum('gnd,gdf->gnf', r, w1, preferred_element_type=F32)
        h3 = jnp.einsum('gnd,gdf->gnf', r, w3, preferred_element_type=F32)
        u = (jax.nn.silu(h1) * h3).astype(BF16)
        e_out = jnp.einsum('gnf,gfd->gnd', u, w2, preferred_element_type=F32).astype(BF16)
        e_out = e_out.reshape(g_loc, ep, cap, d).transpose(1, 0, 2, 3).reshape(ep, g_loc * cap, d)
        comb = jnp.concatenate([jnp.where(sel, p, 0.0).astype(BF16) for p in split3(gate)], axis=1)
        part = jnp.einsum('sqr,srd->sqd', comb, e_out, preferred_element_type=F32)
        part = part.reshape(ep, 3, t, d).sum(axis=1)
        moe = lax.psum_scatter(part, 'ep', scatter_dimension=0)
        y = (h.astype(F32) + moe).astype(BF16)
        return y.reshape(n, s_len, d)

    return jax.shard_map(body, mesh=mesh, in_specs=(tok, tok, tok, rep, rep, rep, rep, rep, rep, exs, exs, exs), out_specs=tok, check_vma=False)
```

```python
import functools

import jax
import jax.numpy as jnp
from jax import lax
from jax.experimental import pallas as pl
from jax.experimental.pallas import tpu as pltpu
from jax.sharding import PartitionSpec as P

EPS = 1e-6
HEAD = 128
F32, BF16 = jnp.float32, jnp.bfloat16


def rms(xf, g):
    return (xf * lax.rsqrt(jnp.mean(xf * xf, axis=-1, keepdims=True) + EPS) * g).astype(BF16)


def attn_kernel(hb, seq, x_ref, g1_ref, g2_ref, wq_ref, wk_ref, wv_ref, wo_ref, h_ref, z_ref, xn_ref, acc_ref):
    i = pl.program_id(0)
    t = x_ref.shape[0]

    @pl.when(i == 0)
    def _():
        xn_ref[...] = rms(x_ref[...].astype(F32), g1_ref[...])
        acc_ref[...] = jnp.zeros_like(acc_ref)

    xn = xn_ref[...]
    q = jnp.dot(xn, wq_ref[...], preferred_element_type=F32).astype(BF16)
    k = jnp.dot(xn, wk_ref[...], preferred_element_type=F32).astype(BF16)
    v = jnp.dot(xn, wv_ref[...], preferred_element_type=F32).astype(BF16)
    row = lax.broadcasted_iota(jnp.int32, (t, t), 0)
    col = lax.broadcasted_iota(jnp.int32, (t, t), 1)
    mask = (row >= col) & (row // seq == col // seq)
    outs = []
    for j in range(hb):
        sl = slice(j * HEAD, (j + 1) * HEAD)
        s = lax.dot_general(q[:, sl], k[:, sl], (((1,), (1,)), ((), ())), preferred_element_type=F32) * HEAD ** -0.5
        s = jnp.where(mask, s, -1e30)
        e = jnp.exp(s - jnp.max(s, axis=-1, keepdims=True))
        p = (e / jnp.sum(e, axis=-1, keepdims=True)).astype(BF16)
        outs.append(jnp.dot(p, v[:, sl], preferred_element_type=F32).astype(BF16))
    o = jnp.concatenate(outs, axis=1)
    acc_ref[...] += jnp.dot(o, wo_ref[...], preferred_element_type=F32)

    @pl.when(i == pl.num_programs(0) - 1)
    def _():
        att = acc_ref[...].astype(BF16)
        h = (x_ref[...].astype(F32) + att.astype(F32)).astype(BF16)
        h_ref[...] = h
        z = rms(h.astype(F32), g2_ref[...])
        kc = z_ref.shape[2]
        for c in range(z_ref.shape[0]):
            z_ref[c] = z[:, c * kc:(c + 1) * kc]


def attention(xf, g1, g2, wq, wk, wv, wo, seq, nz, hb=2):
    t, d = xf.shape
    wid = wq.shape[1]
    c = hb * HEAD
    return pl.pallas_call(
        functools.partial(attn_kernel, hb, seq),
        grid=(wid // c,),
        in_specs=[
            pl.BlockSpec((t, d), lambda i: (0, 0)),
            pl.BlockSpec((1, d), lambda i: (0, 0)),
            pl.BlockSpec((1, d), lambda i: (0, 0)),
            pl.BlockSpec((d, c), lambda i: (0, i)),
            pl.BlockSpec((d, c), lambda i: (0, i)),
            pl.BlockSpec((d, c), lambda i: (0, i)),
            pl.BlockSpec((c, d), lambda i: (i, 0)),
        ],
        out_specs=[pl.BlockSpec((t, d), lambda i: (0, 0)), pl.BlockSpec((nz, t, d // nz), lambda i: (0, 0, 0))],
        out_shape=[jax.ShapeDtypeStruct((t, d), BF16), jax.ShapeDtypeStruct((nz, t, d // nz), BF16)],
        scratch_shapes=[pltpu.VMEM((t, d), BF16), pltpu.VMEM((t, d), F32)],
        compiler_params=pltpu.CompilerParams(dimension_semantics=("arbitrary",), vmem_limit_bytes=48 * 2**20),
        cost_estimate=pl.CostEstimate(flops=8 * t * d * wid, bytes_accessed=8 * d * wid, transcendentals=0),
        name="attention",
    )(xf, g1.reshape(1, d), g2.reshape(1, d), wq, wk, wv, wo)


MESH = pl.DeviceIdType.MESH
NZ, NW, NW2, NCOL = 4, 4, 8, 256


def moe_kernel(ep, cfg, meta_ref, z_ref, h_ref, w1_ref, w3_ref, w2_ref, y_ref,
               mbuf, zbuf, dbuf, gbuf, wbuf, acc1, acc3, rbuf, ubuf, w2buf, ebuf, h1buf, h2buf,
               load_sem, m_send, m_recv, z_send, z_recv, w_sem, w2_sem, r_send, r_recv, ready):
    g_loc, cp, ncol = cfg
    nz, _, t, kc = zbuf.shape
    tp = mbuf.shape[2]
    ff = acc1.shape[2]
    d = nz * kc
    rows = ep * cp
    chips = ep // 2
    half = t // 2
    n2 = d // ncol
    nq = ff // ncol
    nw, nw2 = wbuf.shape[0], w2buf.shape[0]

    me = lax.axis_index('ep')
    chip, core = me // 2, lax.rem(me, 2)
    rchip, lchip, ochip = lax.rem(chip + 1, chips), lax.rem(chip + chips - 1, chips), lax.rem(chip + 2, chips)
    right, left, opp, sib = rchip * 2 + core, lchip * 2 + core, ochip * 2 + core, chip * 2 + 1 - core

    def send(src, dst, ssem, rsem, dev):
        return pltpu.make_async_remote_copy(src_ref=src, dst_ref=dst, send_sem=ssem, recv_sem=rsem,
                                            device_id={'ep': dev}, device_id_type=MESH)

    def wcopy(n, which):
        e, c = lax.rem(n, g_loc), n // g_loc
        ref = w3_ref if which else w1_ref
        slot = lax.rem(n, nw)
        return pltpu.make_async_copy(ref.at[e, pl.ds(c * kc, kc)], wbuf.at[slot, which], w_sem.at[slot, which])

    def w2copy(n):
        e, c = lax.rem(n, g_loc), n // g_loc
        slot = lax.rem(n, nw2)
        return pltpu.make_async_copy(w2_ref.at[e, :, pl.ds(pl.multiple_of(c * ncol, ncol), ncol)], w2buf.at[slot], w2_sem.at[slot])

    zload = pltpu.make_async_copy(z_ref, zbuf.at[:, me], load_sem.at[0])
    mload = pltpu.make_async_copy(meta_ref, mbuf.at[me], load_sem.at[1])
    zload.start()
    mload.start()
    for n in range(nw):
        wcopy(n, 0).start()
        wcopy(n, 1).start()
    for n in range(nw2):
        w2copy(n).start()

    barrier = pltpu.get_barrier_semaphore()
    for dev in (right, left, sib):
        pl.semaphore_signal(barrier, inc=1, device_id={'ep': dev}, device_id_type=MESH)
    pl.semaphore_wait(barrier, 3)

    def mcopy(k):
        who, dev = ((me, right), (me, left), (me, sib), (left, right), (left, sib), (right, sib), (opp, sib))[k]
        return send(mbuf.at[who], mbuf.at[who], m_send.at[k], m_recv.at[k], dev)

    def zcopy(c, k):
        if k == 3:
            ref, dev = zbuf.at[c, left, pl.ds(0, half)], right
        elif k == 4:
            ref, dev = zbuf.at[c, right, pl.ds(half, half)], left
        else:
            who, dev = {0: (me, right), 1: (me, left), 2: (me, sib), 5: (left, sib), 6: (right, sib), 7: (opp, sib)}[k]
            ref = zbuf.at[c, who]
        return send(ref, ref, z_send.at[c, k], z_recv.at[c, k], dev)

    def own(c):
        for k in (0, 1, 2):
            zcopy(c, k).start()

    def stage1(c):
        zcopy(c, 0).wait_recv()
        zcopy(c, 3).start()
        zcopy(c, 5).start()
        zcopy(c, 1).wait_recv()
        zcopy(c, 4).start()
        zcopy(c, 6).start()

    def stage2(c):
        zcopy(c, 3).wait_recv()
        zcopy(c, 4).wait_recv()
        zcopy(c, 7).start()

    def stage3(c):
        for k in (2, 5, 6, 7):
            zcopy(c, k).wait_recv()

    mload.wait()
    for k in (0, 1, 2):
        mcopy(k).start()
    zload.wait()
    own(0)

    def zero(e, _):
        acc1[e] = jnp.zeros_like(acc1[e])
        acc3[e] = jnp.zeros_like(acc3[e])
        return 0

    lax.fori_loop(0, g_loc, zero, 0)
    mcopy(0).wait_recv()
    mcopy(3).start()
    mcopy(4).start()
    mcopy(1).wait_recv()
    mcopy(5).start()
    own(1)
    mcopy(3).wait_recv()
    mcopy(6).start()
    for k in (2, 4, 5, 6):
        mcopy(k).wait_recv()

    base = (me * g_loc).astype(F32)

    def build(s, _):
        m = mbuf[s]
        top = m.shape[0] // 2
        ids, gt = m[:top], m[top:]
        masks, gates = [], []
        for e in range(g_loc):
            hit = ids == base + float(e)
            masks.append(jnp.max(jnp.where(hit, 1.0, 0.0), axis=0, keepdims=True))
            gates.append(jnp.sum(jnp.where(hit, gt, 0.0), axis=0, keepdims=True))
        mask, gate = jnp.concatenate(masks, axis=0), jnp.concatenate(gates, axis=0)
        before = lax.broadcasted_iota(jnp.int32, (tp, tp), 0) < lax.broadcasted_iota(jnp.int32, (tp, tp), 1)
        rank = jnp.dot(mask.astype(BF16), jnp.where(before, 1.0, 0.0).astype(BF16), preferred_element_type=F32)
        place = jnp.where(mask > 0.5, rank, -1.0)
        slot = lax.broadcasted_iota(jnp.int32, (cp, t), 0).astype(F32)
        dbuf[s] = jnp.concatenate([jnp.where(slot == place[e:e + 1, :t], 1.0, 0.0) for e in range(g_loc)], axis=0).astype(BF16)
        re = lax.broadcasted_iota(jnp.int32, (g_loc, g_loc * cp), 0)
        rr = lax.broadcasted_iota(jnp.int32, (g_loc, g_loc * cp), 1)
        spread = jnp.where((rr >= re * cp) & (rr < re * cp + cp), 1.0, 0.0).astype(BF16)

        def widen(a):
            return lax.dot_general(a, spread, (((0,), (0,)), ((), ())), preferred_element_type=F32)[:t]

        slots = lax.rem(lax.broadcasted_iota(jnp.int32, (t, g_loc * cp), 1), cp).astype(F32)
        sel = widen(place.astype(BF16)) == slots
        hi = gate.astype(BF16)
        r1 = gate - hi.astype(F32)
        mid = r1.astype(BF16)
        lo = (r1 - mid.astype(F32)).astype(BF16)
        for i, part in enumerate((hi, mid, lo)):
            gbuf[s, i * t:(i + 1) * t] = jnp.where(sel, widen(part), 0.0).astype(BF16)
        return 0

    stage1(0)
    lax.fori_loop(0, ep // 2, build, 0)
    stage2(0)
    lax.fori_loop(ep // 2, ep, build, 0)

    def dispatch(c):
        def pair(p, _):
            a = jnp.dot(dbuf[2 * p], zbuf[c, 2 * p], preferred_element_type=F32)
            b = jnp.dot(dbuf[2 * p + 1], zbuf[c, 2 * p + 1], preferred_element_type=F32)
            for e in range(g_loc):
                sl = slice(e * cp, (e + 1) * cp)
                rbuf[e, pl.ds(pl.multiple_of(p * 2 * cp, 2 * cp), 2 * cp)] = jnp.concatenate([a[sl], b[sl]], axis=0).astype(BF16)
            return 0

        lax.fori_loop(0, ep // 2, pair, 0)

    def expert_in(c, last):
        def step(e, _):
            n = c * g_loc + e
            slot = lax.rem(n, nw)
            wcopy(n, 0).wait()
            wcopy(n, 1).wait()
            r = rbuf[e]
            a = acc1[e] + jnp.dot(r, wbuf[slot, 0], preferred_element_type=F32)
            b = acc3[e] + jnp.dot(r, wbuf[slot, 1], preferred_element_type=F32)
            if last:
                ubuf[e] = (a / (1.0 + jnp.exp(-a)) * b).astype(BF16)
            else:
                acc1[e] = a
                acc3[e] = b

            @pl.when(n + nw < nz * g_loc)
            def _():
                wcopy(n + nw, 0).start()
                wcopy(n + nw, 1).start()

            return 0

        return step

    def chunk(c, _):
        stage3(c)
        dispatch(c)

        @pl.when(c + 2 < nz)
        def _():
            own(c + 2)

        stage1(c + 1)
        step = expert_in(c, False)
        lax.fori_loop(0, g_loc // 2, step, 0)
        stage2(c + 1)
        lax.fori_loop(g_loc // 2, g_loc, step, 0)
        return 0

    lax.fori_loop(0, nz - 1, chunk, 0)
    stage3(nz - 1)
    dispatch(nz - 1)
    lax.fori_loop(0, g_loc, expert_in(nz - 1, True), 0)
    pl.semaphore_signal(ready, inc=1, device_id={'ep': sib}, device_id_type=MESH)

    def cols(c):
        return pl.ds(pl.multiple_of(lax.rem(c, nq) * ncol, ncol), ncol)

    def rcopy(c, k):
        if k == 0:
            src = acc1.at[pl.ds(chips, chips), pl.ds(0, t), cols(c)]
            dst, dev = acc3.at[pl.ds(c // nq * chips, chips), pl.ds(0, t), cols(c)], sib
        elif k == 1:
            src, dst, dev = acc1.at[ochip, pl.ds(0, half), cols(c)], h1buf.at[c, 0], right
        elif k == 2:
            src, dst, dev = acc1.at[ochip, pl.ds(half, half), cols(c)], h1buf.at[c, 1], left
        elif k == 3:
            src, dst, dev = acc1.at[rchip, pl.ds(0, t), cols(c)], h2buf.at[c, 0], right
        else:
            src, dst, dev = acc1.at[lchip, pl.ds(0, t), cols(c)], h2buf.at[c, 1], left
        return send(src, dst, r_send.at[c, k], r_recv.at[c, k], dev)

    def out_cols(c):
        def step(e, _):
            n = c * g_loc + e
            w2copy(n).wait()
            o = jnp.dot(ubuf[e], w2buf[lax.rem(n, nw2)], preferred_element_type=F32)
            ebuf[e] = o.astype(BF16).astype(F32)

            @pl.when(n + nw2 < n2 * g_loc)
            def _():
                w2copy(n + nw2).start()

            return 0

        lax.fori_loop(0, g_loc, step, 0)

        def comb(s, _):
            at = pl.ds(pl.multiple_of(s * cp, cp), cp)
            es = jnp.concatenate([ebuf[e, at] for e in range(g_loc)], axis=0).astype(BF16)
            p = jnp.dot(gbuf[s], es, preferred_element_type=F32)
            place = s // 2 + jnp.where(lax.rem(s, 2) == core, 0, chips)
            acc1[place, pl.ds(0, t), cols(c)] = p[:t] + p[t:2 * t] + p[2 * t:]
            return 0

        lax.fori_loop(0, ep, comb, 0)

    def stage_b(c):
        rcopy(c, 0).wait_recv()

        def add(j, _):
            acc1[j, pl.ds(0, t), cols(c)] += acc3[c // nq * chips + j, pl.ds(0, t), cols(c)]
            return 0

        lax.fori_loop(0, chips, add, 0)
        rcopy(c, 1).start()
        rcopy(c, 2).start()

    def stage_c(c):
        rcopy(c, 1).wait_recv()
        acc1[rchip, pl.ds(0, half), cols(c)] += h1buf[c, 0]
        rcopy(c, 3).start()
        rcopy(c, 2).wait_recv()
        acc1[lchip, pl.ds(half, half), cols(c)] += h1buf[c, 1]
        rcopy(c, 4).start()

    def stage_d(c):
        rcopy(c, 3).wait_recv()
        rcopy(c, 4).wait_recv()
        moe = acc1[chip, pl.ds(0, t), cols(c)] + h2buf[c, 0] + h2buf[c, 1]
        at = pl.ds(pl.multiple_of(c * ncol, ncol), ncol)
        y_ref[:, at] = (h_ref[:, at].astype(F32) + moe).astype(BF16)
        for k in range(5):
            rcopy(c, k).wait_send()

    def tail_step(i, _):
        @pl.when(i < n2)
        def _():
            out_cols(i)

            @pl.when(i == 0)
            def _():
                pl.semaphore_wait(ready, 1)

            rcopy(i, 0).start()

        @pl.when((i >= 1) & (i - 1 < n2))
        def _():
            stage_b(i - 1)

        @pl.when((i >= 2) & (i - 2 < n2))
        def _():
            stage_c(i - 2)

        @pl.when(i >= 3)
        def _():
            stage_d(i - 3)

        return 0

    lax.fori_loop(0, n2 + 3, tail_step, 0)
    for k in range(7):
        mcopy(k).wait_send()

    def drain(c, _):
        for k in range(8):
            zcopy(c, k).wait_send()
        return 0

    lax.fori_loop(0, nz, drain, 0)


def moe(ep, meta, z, h, w1, w3, w2, cap, ncol):
    nz, t, kc = z.shape
    g_loc, d, ff = w1.shape
    cp = -(-cap // 8) * 8
    rows = ep * cp
    n2 = d // ncol
    vm = lambda *s: pltpu.VMEM(s, BF16)
    vf = lambda *s: pltpu.VMEM(s, F32)
    hbm = pl.BlockSpec(memory_space=pltpu.HBM)
    vmem = pl.BlockSpec(memory_space=pltpu.VMEM)
    dma = pltpu.SemaphoreType.DMA
    return pl.pallas_call(
        functools.partial(moe_kernel, ep, (g_loc, cp, ncol)),
        in_specs=[hbm, hbm, vmem, hbm, hbm, hbm],
        out_specs=vmem,
        out_shape=jax.ShapeDtypeStruct((t, d), BF16),
        scratch_shapes=[
            vf(ep, *meta.shape), vm(nz, ep, t, kc), vm(ep, g_loc * cp, t), vm(ep, 3 * t, g_loc * cp),
            vm(NW, 2, kc, ff), vf(g_loc, rows, ff), vf(g_loc, rows, ff), vm(g_loc, rows, kc), vm(g_loc, rows, ff),
            vm(NW2, ff, ncol), vf(g_loc, rows, ncol), vf(n2, 2, t // 2, ncol), vf(n2, 2, t, ncol),
            dma((2,)), dma((7,)), dma((7,)), dma((nz, 8)), dma((nz, 8)), dma((NW, 2)), dma((NW2,)),
            dma((n2, 5)), dma((n2, 5)), pltpu.SemaphoreType.REGULAR,
        ],
        compiler_params=pltpu.CompilerParams(collective_id=0, has_side_effects=True, vmem_limit_bytes=67043328),
        cost_estimate=pl.CostEstimate(flops=6 * g_loc * rows * d * ff, bytes_accessed=6 * g_loc * d * ff, transcendentals=0),
        name="moe",
    )(meta, z, h, w1, w3, w2)


def solution(mesh):
    ep = mesh.shape['ep']
    tok = P(('dp', 'ep'))
    rep = P()
    exs = P('ep')

    def body(x, idx, gates, g1, wq, wk, wv, wo, g2, w1, w3, w2):
        n, s_len, d = x.shape
        t = n * s_len
        top = idx.shape[-1]
        avg = top * t // (w1.shape[0] * ep)
        cap = avg + avg // 2
        h, z = attention(x.reshape(t, d), g1, g2, wq, wk, wv, wo, s_len, NZ)
        pad = ((0, 0), (0, -t % 128))
        meta = jnp.concatenate([jnp.pad(idx.reshape(t, top).T.astype(F32), pad, constant_values=-1.0),
                                jnp.pad(gates.reshape(t, top).T, pad)], axis=0)
        return moe(ep, meta, z, h, w1, w3, w2, cap, NCOL).reshape(n, s_len, d)

    return jax.shard_map(body, mesh=mesh, in_specs=(tok, tok, tok, rep, rep, rep, rep, rep, rep, exs, exs, exs), out_specs=tok, check_vma=False)
```

```python
import functools

import jax
import jax.numpy as jnp
from jax import lax
from jax.experimental import pallas as pl
from jax.experimental.pallas import tpu as pltpu
from jax.sharding import PartitionSpec as P

EPS = 1e-6
HEAD = 128
F32, BF16 = jnp.float32, jnp.bfloat16


def rms(xf, g):
    return (xf * lax.rsqrt(jnp.mean(xf * xf, axis=-1, keepdims=True) + EPS) * g).astype(BF16)


def split3(g):
    hi = g.astype(BF16)
    r = g - hi.astype(F32)
    mid = r.astype(BF16)
    return hi, mid, (r - mid.astype(F32)).astype(BF16)


def attn_kernel(hb, seq, x_ref, idx_ref, gate_ref, g1_ref, g2_ref, wq_ref, wk_ref, wv_ref, wo_ref, h_ref, z_ref, meta_ref, xn_ref, acc_ref):
    i = pl.program_id(0)
    t = x_ref.shape[0]

    @pl.when(i == 0)
    def _():
        xn_ref[...] = rms(x_ref[...].astype(F32), g1_ref[...])
        acc_ref[...] = jnp.zeros_like(acc_ref)
        top, tp = meta_ref.shape[0] // 2, meta_ref.shape[1]
        at, to = lax.broadcasted_iota(jnp.int32, (t, tp), 0), lax.broadcasted_iota(jnp.int32, (t, tp), 1)
        eye = jnp.where(at == to, 1.0, 0.0).astype(BF16)

        def turn(a):
            return lax.dot_general(a, eye, (((0,), (0,)), ((), ())), preferred_element_type=F32)

        real = lax.broadcasted_iota(jnp.int32, (top, tp), 1) < t
        meta_ref[:top] = jnp.where(real, turn(idx_ref[...].astype(F32).astype(BF16)), -1.0)
        hi, mid, lo = split3(gate_ref[...])
        meta_ref[top:] = turn(hi) + turn(mid) + turn(lo)

    xn = xn_ref[...]
    q = jnp.dot(xn, wq_ref[...], preferred_element_type=F32).astype(BF16)
    k = jnp.dot(xn, wk_ref[...], preferred_element_type=F32).astype(BF16)
    v = jnp.dot(xn, wv_ref[...], preferred_element_type=F32).astype(BF16)
    row = lax.broadcasted_iota(jnp.int32, (t, t), 0)
    col = lax.broadcasted_iota(jnp.int32, (t, t), 1)
    mask = (row >= col) & (row // seq == col // seq)
    outs = []
    for j in range(hb):
        sl = slice(j * HEAD, (j + 1) * HEAD)
        s = lax.dot_general(q[:, sl], k[:, sl], (((1,), (1,)), ((), ())), preferred_element_type=F32) * HEAD ** -0.5
        s = jnp.where(mask, s, -1e30)
        e = jnp.exp(s - jnp.max(s, axis=-1, keepdims=True))
        p = (e / jnp.sum(e, axis=-1, keepdims=True)).astype(BF16)
        outs.append(jnp.dot(p, v[:, sl], preferred_element_type=F32).astype(BF16))
    o = jnp.concatenate(outs, axis=1)
    acc_ref[...] += jnp.dot(o, wo_ref[...], preferred_element_type=F32)

    @pl.when(i == pl.num_programs(0) - 1)
    def _():
        att = acc_ref[...].astype(BF16)
        h = (x_ref[...].astype(F32) + att.astype(F32)).astype(BF16)
        h_ref[...] = h
        z = rms(h.astype(F32), g2_ref[...])
        kc = z_ref.shape[2]
        for c in range(z_ref.shape[0]):
            z_ref[c] = z[:, c * kc:(c + 1) * kc]


def attention(xf, idx, gates, g1, g2, wq, wk, wv, wo, seq, nz, hb):
    t, d = xf.shape
    top, tp = idx.shape[1], t + -t % 128
    wid = wq.shape[1]
    c = hb * HEAD
    return pl.pallas_call(
        functools.partial(attn_kernel, hb, seq),
        grid=(wid // c,),
        in_specs=[
            pl.BlockSpec((t, d), lambda i: (0, 0)),
            pl.BlockSpec((t, top), lambda i: (0, 0)),
            pl.BlockSpec((t, top), lambda i: (0, 0)),
            pl.BlockSpec((1, d), lambda i: (0, 0)),
            pl.BlockSpec((1, d), lambda i: (0, 0)),
            pl.BlockSpec((d, c), lambda i: (0, i)),
            pl.BlockSpec((d, c), lambda i: (0, i)),
            pl.BlockSpec((d, c), lambda i: (0, i)),
            pl.BlockSpec((c, d), lambda i: (i, 0)),
        ],
        out_specs=[pl.BlockSpec((t, d), lambda i: (0, 0)), pl.BlockSpec((nz, t, d // nz), lambda i: (0, 0, 0)),
                   pl.BlockSpec((2 * top, tp), lambda i: (0, 0))],
        out_shape=[jax.ShapeDtypeStruct((t, d), BF16), jax.ShapeDtypeStruct((nz, t, d // nz), BF16),
                   jax.ShapeDtypeStruct((2 * top, tp), F32)],
        scratch_shapes=[pltpu.VMEM((t, d), BF16), pltpu.VMEM((t, d), F32)],
        compiler_params=pltpu.CompilerParams(dimension_semantics=("arbitrary",), vmem_limit_bytes=67043328),
        cost_estimate=pl.CostEstimate(flops=8 * t * d * wid, bytes_accessed=8 * d * wid, transcendentals=0),
        name="attention",
    )(xf, idx, gates, g1.reshape(1, d), g2.reshape(1, d), wq, wk, wv, wo)


MESH = pl.DeviceIdType.MESH
NZ, NW, NW2, NCOL, HB = 8, 6, 8, 256, 4


def moe_kernel(ep, cfg, meta_ref, z_ref, h_hbm, w1_ref, w3_ref, w2_ref, y_ref,
               mbuf, zbuf, dbuf, gbuf, wbuf, acc1, acc3, rbuf, ubuf, w2buf, h1buf, h2buf, h_ref,
               load_sem, m_send, m_recv, z_send, z_recv, w_sem, w2_sem, r_send, r_recv, y_sem, ready):
    g_loc, cp, ncol = cfg
    nz, _, t, kc = zbuf.shape
    tp = mbuf.shape[2]
    ff = acc1.shape[2]
    d = nz * kc
    kw = 2 * kc
    nk = nz // 2
    rows = ep * cp
    chips = ep // 2
    half = t // 2
    n2 = d // ncol
    nq = ff // ncol
    fit = (rows - t) // cp
    assert fit * nq >= ep
    nw, nw2 = wbuf.shape[0], w2buf.shape[0]

    me = lax.axis_index('ep')
    chip, core = me // 2, lax.rem(me, 2)
    rchip, lchip, ochip = lax.rem(chip + 1, chips), lax.rem(chip + chips - 1, chips), lax.rem(chip + 2, chips)
    right, left, opp, sib = rchip * 2 + core, lchip * 2 + core, ochip * 2 + core, chip * 2 + 1 - core

    def send(src, dst, ssem, rsem, dev):
        return pltpu.make_async_remote_copy(src_ref=src, dst_ref=dst, send_sem=ssem, recv_sem=rsem,
                                            device_id={'ep': dev}, device_id_type=MESH)

    def wcopy(n, which):
        e, c = lax.rem(n, g_loc), n // g_loc
        ref = w3_ref if which else w1_ref
        slot = lax.rem(n, nw)
        return pltpu.make_async_copy(ref.at[e, pl.ds(c * kw, kw)], wbuf.at[slot, which], w_sem.at[slot, which])

    def w2copy(n):
        e, c = lax.rem(n, g_loc), n // g_loc
        slot = lax.rem(n, nw2)
        return pltpu.make_async_copy(w2_ref.at[e, :, pl.ds(pl.multiple_of(c * ncol, ncol), ncol)], w2buf.at[slot], w2_sem.at[slot])

    zload = pltpu.make_async_copy(z_ref, zbuf.at[:, me], load_sem.at[0])
    mload = pltpu.make_async_copy(meta_ref, mbuf.at[me], load_sem.at[1])
    hload = pltpu.make_async_copy(h_hbm, h_ref, load_sem.at[2])
    zload.start()
    mload.start()
    hload.start()
    for n in range(nw):
        wcopy(n, 0).start()
        wcopy(n, 1).start()
    for n in range(nw2):
        w2copy(n).start()

    barrier = pltpu.get_barrier_semaphore()
    for dev in (right, left, sib):
        pl.semaphore_signal(barrier, inc=1, device_id={'ep': dev}, device_id_type=MESH)
    pl.semaphore_wait(barrier, 3)

    def mcopy(k):
        who, dev = ((me, right), (me, left), (me, sib), (left, right), (left, sib), (right, sib), (opp, sib))[k]
        return send(mbuf.at[who], mbuf.at[who], m_send.at[k], m_recv.at[k], dev)

    def zcopy(c, k):
        if k == 3:
            ref, dev = zbuf.at[c, left, pl.ds(0, half)], right
        elif k == 4:
            ref, dev = zbuf.at[c, right, pl.ds(half, half)], left
        else:
            who, dev = {0: (me, right), 1: (me, left), 2: (me, sib), 5: (left, sib), 6: (right, sib), 7: (opp, sib)}[k]
            ref = zbuf.at[c, who]
        return send(ref, ref, z_send.at[c, k], z_recv.at[c, k], dev)

    def own(c):
        for k in (0, 1, 2):
            zcopy(c, k).start()

    def stage1(c):
        zcopy(c, 0).wait_recv()
        zcopy(c, 3).start()
        zcopy(c, 5).start()
        zcopy(c, 1).wait_recv()
        zcopy(c, 4).start()
        zcopy(c, 6).start()

    def stage2(c):
        zcopy(c, 3).wait_recv()
        zcopy(c, 4).wait_recv()
        zcopy(c, 7).start()

    def stage3(c):
        for k in (2, 5, 6, 7):
            zcopy(c, k).wait_recv()

    def hop(m):
        @pl.when(m < nz)
        def _():
            stage1(m)

        @pl.when(m + 2 < nz)
        def _():
            own(m + 2)

    def share(m):
        @pl.when(m < nz)
        def _():
            stage2(m)

    mload.wait()
    for k in (0, 1, 2):
        mcopy(k).start()
    zload.wait()
    own(0)
    own(1)

    def zero(e, _):
        acc1[e] = jnp.zeros_like(acc1[e])
        acc3[e] = jnp.zeros_like(acc3[e])
        return 0

    lax.fori_loop(0, g_loc, zero, 0)
    mcopy(0).wait_recv()
    mcopy(3).start()
    mcopy(4).start()
    mcopy(1).wait_recv()
    mcopy(5).start()
    mcopy(3).wait_recv()
    mcopy(6).start()
    hop(0)
    for k in (2, 4, 5, 6):
        mcopy(k).wait_recv()

    base = (me * g_loc).astype(F32)

    def build(s, _):
        m = mbuf[s]
        top = m.shape[0] // 2
        ids, gt = m[:top], m[top:]
        masks, gates = [], []
        for e in range(g_loc):
            hit = ids == base + float(e)
            masks.append(jnp.max(jnp.where(hit, 1.0, 0.0), axis=0, keepdims=True))
            gates.append(jnp.sum(jnp.where(hit, gt, 0.0), axis=0, keepdims=True))
        mask, gate = jnp.concatenate(masks, axis=0), jnp.concatenate(gates, axis=0)
        before = lax.broadcasted_iota(jnp.int32, (tp, tp), 0) < lax.broadcasted_iota(jnp.int32, (tp, tp), 1)
        rank = jnp.dot(mask.astype(BF16), jnp.where(before, 1.0, 0.0).astype(BF16), preferred_element_type=F32)
        place = jnp.where(mask > 0.5, rank, -1.0)
        slot = lax.broadcasted_iota(jnp.int32, (cp, t), 0).astype(F32)
        dbuf[s] = jnp.concatenate([jnp.where(slot == place[e:e + 1, :t], 1.0, 0.0) for e in range(g_loc)], axis=0).astype(BF16)
        re = lax.broadcasted_iota(jnp.int32, (g_loc, g_loc * cp), 0)
        rr = lax.broadcasted_iota(jnp.int32, (g_loc, g_loc * cp), 1)
        spread = jnp.where((rr >= re * cp) & (rr < re * cp + cp), 1.0, 0.0).astype(BF16)

        def widen(a):
            return lax.dot_general(a, spread, (((0,), (0,)), ((), ())), preferred_element_type=F32)[:t]

        slots = lax.rem(lax.broadcasted_iota(jnp.int32, (t, g_loc * cp), 1), cp).astype(F32)
        sel = widen(place.astype(BF16)) == slots
        for i, part in enumerate(split3(gate)):
            gbuf[s, i * t:(i + 1) * t] = jnp.where(sel, widen(part), 0.0).astype(BF16)
        return 0

    quarter = ep // 4
    lax.fori_loop(0, quarter, build, 0)
    hop(1)
    lax.fori_loop(quarter, 2 * quarter, build, 0)
    share(0)
    lax.fori_loop(2 * quarter, 3 * quarter, build, 0)
    hop(2)
    lax.fori_loop(3 * quarter, ep, build, 0)
    share(1)

    def dispatch(c):
        def pair(p, _):
            for q in range(2):
                a = jnp.dot(dbuf[2 * p], zbuf[2 * c + q, 2 * p], preferred_element_type=F32)
                b = jnp.dot(dbuf[2 * p + 1], zbuf[2 * c + q, 2 * p + 1], preferred_element_type=F32)
                for e in range(g_loc):
                    sl = slice(e * cp, (e + 1) * cp)
                    rbuf[e, pl.ds(pl.multiple_of(p * 2 * cp, 2 * cp), 2 * cp), q * kc:(q + 1) * kc] = (
                        jnp.concatenate([a[sl], b[sl]], axis=0).astype(BF16))
            return 0

        lax.fori_loop(0, ep // 2, pair, 0)

    def experts_in(c, last):
        def step(i, _):
            n = c * g_loc + 2 * i
            for q in range(2):
                wcopy(n + q, 0).wait()
                wcopy(n + q, 1).wait()
            for q in range(2):
                e, slot = 2 * i + q, lax.rem(n + q, nw)
                r = rbuf[e]
                a = acc1[e] + jnp.dot(r, wbuf[slot, 0], preferred_element_type=F32)
                b = acc3[e] + jnp.dot(r, wbuf[slot, 1], preferred_element_type=F32)
                if last:
                    ubuf[e] = (a / (1.0 + jnp.exp(-a)) * b).astype(BF16)
                else:
                    acc1[e] = a
                    acc3[e] = b

            @pl.when(n + nw < nk * g_loc)
            def _():
                for q in range(2):
                    wcopy(n + q + nw, 0).start()
                    wcopy(n + q + nw, 1).start()

            return 0

        return step

    def chunk(c, _):
        stage3(2 * c)
        stage3(2 * c + 1)
        dispatch(c)
        step = experts_in(c, False)

        def portion(i, _):
            @pl.when(i > 0)
            def _():
                hop(2 * c + 2 + i)
                share(2 * c + 1 + i)

            return lax.fori_loop(i * 2 - jnp.minimum(i, 1), jnp.minimum(i * 2 + 1, g_loc // 2), step, 0)

        lax.fori_loop(0, 3, portion, 0)
        return 0

    lax.fori_loop(0, nk - 1, chunk, 0)
    stage3(nz - 2)
    stage3(nz - 1)
    dispatch(nk - 1)
    lax.fori_loop(0, g_loc // 2, experts_in(nk - 1, True), 0)
    hload.wait()
    pl.semaphore_signal(ready, inc=1, device_id={'ep': sib}, device_id_type=MESH)

    def cols(c):
        return pl.ds(pl.multiple_of(lax.rem(c, nq) * ncol, ncol), ncol)

    def rcopy(c, k):
        if k == 0:
            src = acc1.at[pl.ds(chips, chips), pl.ds(0, t), cols(c)]
            dst, dev = acc3.at[pl.ds(c // nq * chips, chips), pl.ds(0, t), cols(c)], sib
        elif k == 1:
            src, dst, dev = acc1.at[ochip, pl.ds(0, half), cols(c)], h1buf.at[c, 0], right
        elif k == 2:
            src, dst, dev = acc1.at[ochip, pl.ds(half, half), cols(c)], h1buf.at[c, 1], left
        elif k == 3:
            src, dst, dev = acc1.at[rchip, pl.ds(0, t), cols(c)], h2buf.at[c, 0], right
        else:
            src, dst, dev = acc1.at[lchip, pl.ds(0, t), cols(c)], h2buf.at[c, 1], left
        return send(src, dst, r_send.at[c, k], r_recv.at[c, k], dev)

    def out_cols(c):
        def step(i, _):
            n = c * g_loc + 4 * i
            for q in range(4):
                w2copy(n + q).wait()
            for q in range(4):
                e = 4 * i + q
                o = jnp.dot(ubuf[e], w2buf[lax.rem(n + q, nw2)], preferred_element_type=F32)
                o = o.astype(BF16).astype(F32)
                for r in range(ep):
                    acc3[e, t + r % fit * cp:t + (r % fit + 1) * cp, r // fit * ncol:(r // fit + 1) * ncol] = o[r * cp:(r + 1) * cp]

            @pl.when(n + nw2 < n2 * g_loc)
            def _():
                for q in range(4):
                    w2copy(n + q + nw2).start()

            return 0

        lax.fori_loop(0, g_loc // 4, step, 0)

        def comb(i, _):
            for q in range(4):
                s = 4 * i + q
                at = pl.ds(pl.multiple_of(t + lax.rem(s, fit) * cp, 8), cp), pl.ds(pl.multiple_of(s // fit * ncol, ncol), ncol)
                es = jnp.concatenate([acc3[e, at[0], at[1]] for e in range(g_loc)], axis=0).astype(BF16)
                p = jnp.dot(gbuf[s], es, preferred_element_type=F32)
                place = s // 2 + jnp.where(q % 2 == core, 0, chips)
                acc1[place, pl.ds(0, t), cols(c)] = p[:t] + p[t:2 * t] + p[2 * t:]
            return 0

        lax.fori_loop(0, ep // 4, comb, 0)

    def stage_b(c):
        rcopy(c, 0).wait_recv()

        def add(j, _):
            acc1[j, pl.ds(0, t), cols(c)] += acc3[c // nq * chips + j, pl.ds(0, t), cols(c)]
            return 0

        lax.fori_loop(0, chips, add, 0)
        rcopy(c, 1).start()
        rcopy(c, 2).start()

    def stage_c(c):
        rcopy(c, 1).wait_recv()
        acc1[rchip, pl.ds(0, half), cols(c)] += h1buf[c, 0]
        rcopy(c, 3).start()
        rcopy(c, 2).wait_recv()
        acc1[lchip, pl.ds(half, half), cols(c)] += h1buf[c, 1]
        rcopy(c, 4).start()

    def ycopy(c):
        at = pl.ds(pl.multiple_of(c * ncol, ncol), ncol)
        return pltpu.make_async_copy(h_ref.at[:, at], y_ref.at[:, at], y_sem.at[c])

    def stage_d(c):
        rcopy(c, 3).wait_recv()
        rcopy(c, 4).wait_recv()
        moe = acc1[chip, pl.ds(0, t), cols(c)] + h2buf[c, 0] + h2buf[c, 1]
        at = pl.ds(pl.multiple_of(c * ncol, ncol), ncol)
        h_ref[:, at] = (h_ref[:, at].astype(F32) + moe).astype(BF16)
        ycopy(c).start()
        for k in range(5):
            rcopy(c, k).wait_send()

    def tail_step(i, _):
        @pl.when(i < n2)
        def _():
            out_cols(i)

            @pl.when(i == 0)
            def _():
                pl.semaphore_wait(ready, 1)

            rcopy(i, 0).start()

        @pl.when((i >= 1) & (i - 1 < n2))
        def _():
            stage_b(i - 1)

        @pl.when((i >= 2) & (i - 2 < n2))
        def _():
            stage_c(i - 2)

        @pl.when(i >= 3)
        def _():
            stage_d(i - 3)

        return 0

    lax.fori_loop(0, n2 + 3, tail_step, 0)
    for k in range(7):
        mcopy(k).wait_send()

    def drain(c, _):
        for k in range(8):
            zcopy(c, k).wait_send()
        return 0

    lax.fori_loop(0, nz, drain, 0)

    def finish(c, _):
        ycopy(c).wait()
        return 0

    lax.fori_loop(0, n2, finish, 0)


def moe(ep, meta, z, h, w1, w3, w2, cap, ncol):
    nz, t, kc = z.shape
    g_loc, d, ff = w1.shape
    cp = -(-cap // 8) * 8
    rows = ep * cp
    n2 = d // ncol
    vm = lambda *s: pltpu.VMEM(s, BF16)
    vf = lambda *s: pltpu.VMEM(s, F32)
    hbm = pl.BlockSpec(memory_space=pltpu.HBM)
    dma = pltpu.SemaphoreType.DMA
    return pl.pallas_call(
        functools.partial(moe_kernel, ep, (g_loc, cp, ncol)),
        in_specs=[hbm] * 6,
        out_specs=hbm,
        out_shape=jax.ShapeDtypeStruct((t, d), BF16),
        scratch_shapes=[
            vf(ep, *meta.shape), vm(nz, ep, t, kc), vm(ep, g_loc * cp, t), vm(ep, 3 * t, g_loc * cp),
            vm(NW, 2, 2 * kc, ff), vf(g_loc, rows, ff), vf(g_loc, rows, ff), vm(g_loc, rows, 2 * kc), vm(g_loc, rows, ff),
            vm(NW2, ff, ncol), vf(n2, 2, t // 2, ncol), vf(n2, 2, t, ncol), vm(t, d),
            dma((3,)), dma((7,)), dma((7,)), dma((nz, 8)), dma((nz, 8)), dma((NW, 2)), dma((NW2,)),
            dma((n2, 5)), dma((n2, 5)), dma((n2,)), pltpu.SemaphoreType.REGULAR,
        ],
        compiler_params=pltpu.CompilerParams(collective_id=0, has_side_effects=True, vmem_limit_bytes=67043328),
        cost_estimate=pl.CostEstimate(flops=6 * g_loc * rows * d * ff, bytes_accessed=6 * g_loc * d * ff, transcendentals=0),
        name="moe",
    )(meta, z, h, w1, w3, w2)


def solution(mesh):
    ep = mesh.shape['ep']
    tok = P(('dp', 'ep'))
    rep = P()
    exs = P('ep')

    def body(x, idx, gates, g1, wq, wk, wv, wo, g2, w1, w3, w2):
        n, s_len, d = x.shape
        t = n * s_len
        top = idx.shape[-1]
        avg = top * t // (w1.shape[0] * ep)
        cap = avg + avg // 2
        h, z, meta = attention(x.reshape(t, d), idx.reshape(t, top), gates.reshape(t, top), g1, g2, wq, wk, wv, wo, s_len, NZ, HB)
        return moe(ep, meta, z, h, w1, w3, w2, cap, NCOL).reshape(n, s_len, d)

    return jax.shard_map(body, mesh=mesh, in_specs=(tok, tok, tok, rep, rep, rep, rep, rep, rep, exs, exs, exs), out_specs=tok, check_vma=False)
```

```python
import functools

import jax
import jax.numpy as jnp
from jax import lax
from jax.experimental import pallas as pl
from jax.experimental.pallas import tpu as pltpu
from jax.sharding import PartitionSpec as P

EPS = 1e-6
HEAD = 128
F32, BF16 = jnp.float32, jnp.bfloat16


def rms(xf, g):
    return (xf * lax.rsqrt(jnp.mean(xf * xf, axis=-1, keepdims=True) + EPS) * g).astype(BF16)


def split3(g):
    hi = g.astype(BF16)
    r = g - hi.astype(F32)
    mid = r.astype(BF16)
    return hi, mid, (r - mid.astype(F32)).astype(BF16)


def attn_kernel(hb, seq, x_ref, idx_ref, gate_ref, g1_ref, g2_ref, wq_ref, wk_ref, wv_ref, wo_ref, h_ref, z_ref, meta_ref, xn_ref, acc_ref):
    i = pl.program_id(0)
    t = x_ref.shape[0]

    @pl.when(i == 0)
    def _():
        xn_ref[...] = rms(x_ref[...].astype(F32), g1_ref[...])
        acc_ref[...] = jnp.zeros_like(acc_ref)
        top, tp = meta_ref.shape[0] // 2, meta_ref.shape[1]
        ids, gts = jnp.zeros((top, tp), F32), jnp.zeros((top, tp), F32)
        for n in range(t // seq):
            at, to = lax.broadcasted_iota(jnp.int32, (seq, tp), 0), lax.broadcasted_iota(jnp.int32, (seq, tp), 1)
            move = jnp.where(at + n * seq == to, 1.0, 0.0).astype(BF16)
            ids += jnp.dot(idx_ref[n].astype(F32).astype(BF16), move, preferred_element_type=F32)
            hi, mid, lo = [jnp.dot(p, move, preferred_element_type=F32) for p in split3(gate_ref[n])]
            gts += hi + mid + lo
        meta_ref[:top] = jnp.where(lax.broadcasted_iota(jnp.int32, (top, tp), 1) < t, ids, -1.0)
        meta_ref[top:] = gts

    xn = xn_ref[...]
    q = jnp.dot(xn, wq_ref[...], preferred_element_type=F32).astype(BF16)
    k = jnp.dot(xn, wk_ref[...], preferred_element_type=F32).astype(BF16)
    v = jnp.dot(xn, wv_ref[...], preferred_element_type=F32).astype(BF16)
    row = lax.broadcasted_iota(jnp.int32, (t, t), 0)
    col = lax.broadcasted_iota(jnp.int32, (t, t), 1)
    mask = (row >= col) & (row // seq == col // seq)
    outs = []
    for j in range(hb):
        sl = slice(j * HEAD, (j + 1) * HEAD)
        s = lax.dot_general(q[:, sl], k[:, sl], (((1,), (1,)), ((), ())), preferred_element_type=F32) * HEAD ** -0.5
        s = jnp.where(mask, s, -1e30)
        e = jnp.exp(s - jnp.max(s, axis=-1, keepdims=True))
        p = (e / jnp.sum(e, axis=-1, keepdims=True)).astype(BF16)
        outs.append(jnp.dot(p, v[:, sl], preferred_element_type=F32).astype(BF16))
    o = jnp.concatenate(outs, axis=1)
    acc_ref[...] += jnp.dot(o, wo_ref[...], preferred_element_type=F32)

    @pl.when(i == pl.num_programs(0) - 1)
    def _():
        att = acc_ref[...].astype(BF16)
        h = (x_ref[...].astype(F32) + att.astype(F32)).astype(BF16)
        h_ref[...] = h
        z = rms(h.astype(F32), g2_ref[...])
        kc = z_ref.shape[2]
        for c in range(z_ref.shape[0]):
            z_ref[c] = z[:, c * kc:(c + 1) * kc]


def attention(xf, idx, gates, g1, g2, wq, wk, wv, wo, seq, nz, hb):
    t, d = xf.shape
    n, top, _ = idx.shape
    tp = t + -t % 128
    wid = wq.shape[1]
    c = hb * HEAD
    return pl.pallas_call(
        functools.partial(attn_kernel, hb, seq),
        grid=(wid // c,),
        in_specs=[
            pl.BlockSpec((t, d), lambda i: (0, 0)),
            pl.BlockSpec((n, top, seq), lambda i: (0, 0, 0)),
            pl.BlockSpec((n, top, seq), lambda i: (0, 0, 0)),
            pl.BlockSpec((1, d), lambda i: (0, 0)),
            pl.BlockSpec((1, d), lambda i: (0, 0)),
            pl.BlockSpec((d, c), lambda i: (0, i)),
            pl.BlockSpec((d, c), lambda i: (0, i)),
            pl.BlockSpec((d, c), lambda i: (0, i)),
            pl.BlockSpec((c, d), lambda i: (i, 0)),
        ],
        out_specs=[pl.BlockSpec((t, d), lambda i: (0, 0)), pl.BlockSpec((nz, t, d // nz), lambda i: (0, 0, 0)),
                   pl.BlockSpec((2 * top, tp), lambda i: (0, 0))],
        out_shape=[jax.ShapeDtypeStruct((t, d), BF16), jax.ShapeDtypeStruct((nz, t, d // nz), BF16),
                   jax.ShapeDtypeStruct((2 * top, tp), F32)],
        scratch_shapes=[pltpu.VMEM((t, d), BF16), pltpu.VMEM((t, d), F32)],
        compiler_params=pltpu.CompilerParams(dimension_semantics=("arbitrary",), vmem_limit_bytes=67043328),
        cost_estimate=pl.CostEstimate(flops=8 * t * d * wid, bytes_accessed=8 * d * wid, transcendentals=0),
        name="attention",
    )(xf, idx, gates, g1.reshape(1, d), g2.reshape(1, d), wq, wk, wv, wo)


MESH = pl.DeviceIdType.MESH
NZ, NW, NW2, NCOL, HB = 8, 6, 8, 256, 4


def moe_kernel(ep, cfg, meta_ref, z_ref, h_hbm, w1_ref, w3_ref, w2_ref, y_ref,
               mbuf, zbuf, dbuf, gbuf, wbuf, acc1, acc3, rbuf, ubuf, w2buf, h1buf, h2buf, h_ref,
               load_sem, m_send, m_recv, z_send, z_recv, w_sem, w2_sem, r_send, r_recv, y_sem, ready):
    g_loc, cp, ncol = cfg
    nz, _, t, kc = zbuf.shape
    tp = mbuf.shape[2]
    ff = acc1.shape[2]
    d = nz * kc
    kw = 2 * kc
    nk = nz // 2
    rows = ep * cp
    chips = ep // 2
    half = t // 2
    n2 = d // ncol
    nq = ff // ncol
    fit = (rows - t) // cp
    assert fit * nq >= ep
    nw, nw2 = wbuf.shape[0], w2buf.shape[0]

    me = lax.axis_index('ep')
    chip, core = me // 2, lax.rem(me, 2)
    rchip, lchip, ochip = lax.rem(chip + 1, chips), lax.rem(chip + chips - 1, chips), lax.rem(chip + 2, chips)
    right, left, opp, sib = rchip * 2 + core, lchip * 2 + core, ochip * 2 + core, chip * 2 + 1 - core

    def send(src, dst, ssem, rsem, dev):
        return pltpu.make_async_remote_copy(src_ref=src, dst_ref=dst, send_sem=ssem, recv_sem=rsem,
                                            device_id={'ep': dev}, device_id_type=MESH)

    def wcopy(n, which, unit):
        e, c = lax.rem(n, g_loc), n // g_loc
        ref = w3_ref if which else w1_ref
        slot = lax.rem(n, nw)
        row = pl.multiple_of((jnp.maximum(2 * c - 1, 0) + unit) * kc, kc)
        return pltpu.make_async_copy(ref.at[e, pl.ds(row, kc)], wbuf.at[slot, which, unit * kc:(unit + 1) * kc],
                                     w_sem.at[slot, which, unit])

    def wstart(n):
        @pl.when(n < (nk + 1) * g_loc)
        def _():
            wcopy(n, 0, 0).start()
            wcopy(n, 1, 0).start()

        @pl.when((n >= g_loc) & (n < nk * g_loc))
        def _():
            wcopy(n, 0, 1).start()
            wcopy(n, 1, 1).start()

    def w2copy(n):
        e, c = lax.rem(n, g_loc), n // g_loc
        slot = lax.rem(n, nw2)
        return pltpu.make_async_copy(w2_ref.at[e, :, pl.ds(pl.multiple_of(c * ncol, ncol), ncol)], w2buf.at[slot], w2_sem.at[slot])

    zload = pltpu.make_async_copy(z_ref, zbuf.at[:, me], load_sem.at[0])
    mload = pltpu.make_async_copy(meta_ref, mbuf.at[me], load_sem.at[1])
    hload = pltpu.make_async_copy(h_hbm, h_ref, load_sem.at[2])
    zload.start()
    mload.start()
    hload.start()
    for n in range(nw):
        wstart(n)
    for n in range(nw2):
        w2copy(n).start()

    barrier = pltpu.get_barrier_semaphore()
    for k in range(1, ep):
        pl.semaphore_signal(barrier, inc=1, device_id={'ep': lax.rem(me + k, ep)}, device_id_type=MESH)
    mload.wait()
    pl.semaphore_wait(barrier, ep - 1)

    def mcopy(k):
        return send(mbuf.at[me], mbuf.at[me], m_send.at[k - 1], m_recv.at[k - 1], lax.rem(me + k, ep))

    def zcopy(c, k):
        if k == 3:
            ref, dev = zbuf.at[c, left, pl.ds(0, half)], right
        elif k == 4:
            ref, dev = zbuf.at[c, right, pl.ds(half, half)], left
        else:
            who, dev = {0: (me, right), 1: (me, left), 2: (me, sib), 5: (left, sib), 6: (right, sib), 7: (opp, sib)}[k]
            ref = zbuf.at[c, who]
        return send(ref, ref, z_send.at[c, k], z_recv.at[c, k], dev)

    def own(c):
        for k in (0, 1, 2):
            zcopy(c, k).start()

    def stage1(c):
        zcopy(c, 0).wait_recv()
        zcopy(c, 3).start()
        zcopy(c, 5).start()
        zcopy(c, 1).wait_recv()
        zcopy(c, 4).start()
        zcopy(c, 6).start()

    def stage2(c):
        zcopy(c, 3).wait_recv()
        zcopy(c, 4).wait_recv()
        zcopy(c, 7).start()

    def stage3(c):
        for k in (2, 5, 6, 7):
            zcopy(c, k).wait_recv()

    def hop(m):
        @pl.when(m < nz)
        def _():
            stage1(m)

        @pl.when(m + 2 < nz)
        def _():
            own(m + 2)

    def share(m):
        @pl.when(m < nz)
        def _():
            stage2(m)

    for k in range(1, ep):
        mcopy(k).start()
    zload.wait()
    own(0)
    own(1)
    for k in range(1, ep):
        mcopy(k).wait_recv()

    base = (me * g_loc).astype(F32)

    def build(s):
        m = mbuf[s]
        top = m.shape[0] // 2
        ids, gt = m[:top], m[top:]
        masks, gates = [], []
        for e in range(g_loc):
            hit = ids == base + float(e)
            masks.append(jnp.max(jnp.where(hit, 1.0, 0.0), axis=0, keepdims=True))
            gates.append(jnp.sum(jnp.where(hit, gt, 0.0), axis=0, keepdims=True))
        mask, gate = jnp.concatenate(masks, axis=0), jnp.concatenate(gates, axis=0)
        before = lax.broadcasted_iota(jnp.int32, (tp, tp), 0) < lax.broadcasted_iota(jnp.int32, (tp, tp), 1)
        rank = jnp.dot(mask.astype(BF16), jnp.where(before, 1.0, 0.0).astype(BF16), preferred_element_type=F32)
        place = jnp.where(mask > 0.5, rank, -1.0)
        slot = lax.broadcasted_iota(jnp.int32, (cp, t), 0).astype(F32)
        dbuf[s] = jnp.concatenate([jnp.where(slot == place[e:e + 1, :t], 1.0, 0.0) for e in range(g_loc)], axis=0).astype(BF16)
        re = lax.broadcasted_iota(jnp.int32, (g_loc, g_loc * cp), 0)
        rr = lax.broadcasted_iota(jnp.int32, (g_loc, g_loc * cp), 1)
        spread = jnp.where((rr >= re * cp) & (rr < re * cp + cp), 1.0, 0.0).astype(BF16)

        def widen(a):
            return lax.dot_general(a, spread, (((0,), (0,)), ((), ())), preferred_element_type=F32)[:t]

        slots = lax.rem(lax.broadcasted_iota(jnp.int32, (t, g_loc * cp), 1), cp).astype(F32)
        sel = widen(place.astype(BF16)) == slots
        for i, part in enumerate(split3(gate)):
            gbuf[s, i * t:(i + 1) * t] = jnp.where(sel, widen(part), 0.0).astype(BF16)

    def builds(i, _):
        hop(i)
        for q in range(4):
            build(4 * i + q)
        return 0

    lax.fori_loop(0, ep // 4, builds, 0)
    share(0)

    def dispatch(m, q):
        stage3(m)
        at = pl.ds(pl.multiple_of(q * kc, kc), kc)
        for p in range(ep // 2):
            a = jnp.dot(dbuf[2 * p], zbuf[m, 2 * p], preferred_element_type=F32)
            b = jnp.dot(dbuf[2 * p + 1], zbuf[m, 2 * p + 1], preferred_element_type=F32)
            for e in range(g_loc):
                sl = slice(e * cp, (e + 1) * cp)
                rbuf[e, p * 2 * cp:(p + 1) * 2 * cp, at] = jnp.concatenate([a[sl], b[sl]], axis=0).astype(BF16)

    def experts_in(c, kind):
        units = 2 if kind == 'mid' else 1
        k = units * kc

        def step(i, _):
            n = c * g_loc + 2 * i
            for q in range(2):
                for u in range(units):
                    wcopy(n + q, 0, u).wait()
                    wcopy(n + q, 1, u).wait()
            for q in range(2):
                e, slot = 2 * i + q, lax.rem(n + q, nw)
                r = rbuf[e, :, :k]
                a = jnp.dot(r, wbuf[slot, 0, :k], preferred_element_type=F32)
                b = jnp.dot(r, wbuf[slot, 1, :k], preferred_element_type=F32)
                if kind != 'first':
                    a = acc1[e] + a
                    b = acc3[e] + b
                if kind == 'last':
                    ubuf[e] = (a / (1.0 + jnp.exp(-a)) * b).astype(BF16)
                else:
                    acc1[e] = a
                    acc3[e] = b
            wstart(n + nw)
            wstart(n + nw + 1)
            return 0

        return step

    dispatch(0, 0)

    def opening(i, _):
        @pl.when(i > 0)
        def _():
            hop(2)
            share(1)

        return lax.fori_loop(i * 2, i * 2 + 2, experts_in(0, 'first'), 0)

    lax.fori_loop(0, g_loc // 4, opening, 0)
    hop(3)
    share(2)

    def chunk(c, _):
        def pick(q, _):
            dispatch(2 * c - 1 + q, q)
            return 0

        lax.fori_loop(0, 2, pick, 0)
        step = experts_in(c, 'mid')

        def portion(i, _):
            @pl.when(i > 0)
            def _():
                hop(2 * c + 1 + i)
                share(2 * c + i)

            return lax.fori_loop(i * 2 - jnp.minimum(i, 1), jnp.minimum(i * 2 + 1, g_loc // 2), step, 0)

        lax.fori_loop(0, 3, portion, 0)
        return 0

    lax.fori_loop(1, nk, chunk, 0)
    dispatch(nz - 1, 0)
    lax.fori_loop(0, g_loc // 2, experts_in(nk, 'last'), 0)
    hload.wait()
    pl.semaphore_signal(ready, inc=1, device_id={'ep': sib}, device_id_type=MESH)

    def cols(c):
        return pl.ds(pl.multiple_of(lax.rem(c, nq) * ncol, ncol), ncol)

    def rcopy(c, k):
        if k == 0:
            src = acc1.at[pl.ds(chips, chips), pl.ds(0, t), cols(c)]
            dst, dev = acc3.at[pl.ds(c // nq * chips, chips), pl.ds(0, t), cols(c)], sib
        elif k == 1:
            src, dst, dev = acc1.at[ochip, pl.ds(0, half), cols(c)], h1buf.at[c, 0], right
        elif k == 2:
            src, dst, dev = acc1.at[ochip, pl.ds(half, half), cols(c)], h1buf.at[c, 1], left
        elif k == 3:
            src, dst, dev = acc1.at[rchip, pl.ds(0, t), cols(c)], h2buf.at[c, 0], right
        else:
            src, dst, dev = acc1.at[lchip, pl.ds(0, t), cols(c)], h2buf.at[c, 1], left
        return send(src, dst, r_send.at[c, k], r_recv.at[c, k], dev)

    def out_cols(c):
        def step(i, _):
            n = c * g_loc + 4 * i
            for q in range(4):
                w2copy(n + q).wait()
            for q in range(4):
                e = 4 * i + q
                o = jnp.dot(ubuf[e], w2buf[lax.rem(n + q, nw2)], preferred_element_type=F32)
                o = o.astype(BF16).astype(F32)
                for r in range(ep):
                    acc3[e, t + r % fit * cp:t + (r % fit + 1) * cp, r // fit * ncol:(r // fit + 1) * ncol] = o[r * cp:(r + 1) * cp]

            @pl.when(n + nw2 < n2 * g_loc)
            def _():
                for q in range(4):
                    w2copy(n + q + nw2).start()

            return 0

        lax.fori_loop(0, g_loc // 4, step, 0)

        def comb(i, _):
            for q in range(4):
                s = 4 * i + q
                at = pl.ds(pl.multiple_of(t + lax.rem(s, fit) * cp, 8), cp), pl.ds(pl.multiple_of(s // fit * ncol, ncol), ncol)
                es = jnp.concatenate([acc3[e, at[0], at[1]] for e in range(g_loc)], axis=0).astype(BF16)
                p = jnp.dot(gbuf[s], es, preferred_element_type=F32)
                place = s // 2 + jnp.where(q % 2 == core, 0, chips)
                acc1[place, pl.ds(0, t), cols(c)] = p[:t] + p[t:2 * t] + p[2 * t:]
            return 0

        lax.fori_loop(0, ep // 4, comb, 0)

    def stage_b(c):
        rcopy(c, 0).wait_recv()

        def add(j, _):
            acc1[j, pl.ds(0, t), cols(c)] += acc3[c // nq * chips + j, pl.ds(0, t), cols(c)]
            return 0

        lax.fori_loop(0, chips, add, 0)
        rcopy(c, 1).start()
        rcopy(c, 2).start()

    def stage_c(c):
        rcopy(c, 1).wait_recv()
        acc1[rchip, pl.ds(0, half), cols(c)] += h1buf[c, 0]
        rcopy(c, 3).start()
        rcopy(c, 2).wait_recv()
        acc1[lchip, pl.ds(half, half), cols(c)] += h1buf[c, 1]
        rcopy(c, 4).start()

    def ycopy(c):
        at = pl.ds(pl.multiple_of(c * ncol, ncol), ncol)
        return pltpu.make_async_copy(h_ref.at[:, at], y_ref.at[:, at], y_sem.at[c])

    def stage_d(c):
        rcopy(c, 3).wait_recv()
        rcopy(c, 4).wait_recv()
        moe = acc1[chip, pl.ds(0, t), cols(c)] + h2buf[c, 0] + h2buf[c, 1]
        at = pl.ds(pl.multiple_of(c * ncol, ncol), ncol)
        h_ref[:, at] = (h_ref[:, at].astype(F32) + moe).astype(BF16)
        ycopy(c).start()
        for k in range(5):
            rcopy(c, k).wait_send()

    def tail_step(i, _):
        @pl.when(i < n2)
        def _():
            out_cols(i)

            @pl.when(i == 0)
            def _():
                pl.semaphore_wait(ready, 1)

            rcopy(i, 0).start()

        @pl.when((i >= 1) & (i - 1 < n2))
        def _():
            stage_b(i - 1)

        @pl.when((i >= 2) & (i - 2 < n2))
        def _():
            stage_c(i - 2)

        @pl.when(i >= 3)
        def _():
            stage_d(i - 3)

        return 0

    lax.fori_loop(0, n2 + 3, tail_step, 0)
    for k in range(1, ep):
        mcopy(k).wait_send()

    def drain(c, _):
        for k in range(8):
            zcopy(c, k).wait_send()
        return 0

    lax.fori_loop(0, nz, drain, 0)

    def finish(c, _):
        ycopy(c).wait()
        return 0

    lax.fori_loop(0, n2, finish, 0)


def moe(ep, meta, z, h, w1, w3, w2, cap, ncol):
    nz, t, kc = z.shape
    g_loc, d, ff = w1.shape
    cp = -(-cap // 8) * 8
    rows = ep * cp
    n2 = d // ncol
    vm = lambda *s: pltpu.VMEM(s, BF16)
    vf = lambda *s: pltpu.VMEM(s, F32)
    hbm = pl.BlockSpec(memory_space=pltpu.HBM)
    dma = pltpu.SemaphoreType.DMA
    return pl.pallas_call(
        functools.partial(moe_kernel, ep, (g_loc, cp, ncol)),
        in_specs=[hbm] * 6,
        out_specs=hbm,
        out_shape=jax.ShapeDtypeStruct((t, d), BF16),
        scratch_shapes=[
            vf(ep, *meta.shape), vm(nz, ep, t, kc), vm(ep, g_loc * cp, t), vm(ep, 3 * t, g_loc * cp),
            vm(NW, 2, 2 * kc, ff), vf(g_loc, rows, ff), vf(g_loc, rows, ff), vm(g_loc, rows, 2 * kc), vm(g_loc, rows, ff),
            vm(NW2, ff, ncol), vf(n2, 2, t // 2, ncol), vf(n2, 2, t, ncol), vm(t, d),
            dma((3,)), dma((7,)), dma((7,)), dma((nz, 8)), dma((nz, 8)), dma((NW, 2, 2)), dma((NW2,)),
            dma((n2, 5)), dma((n2, 5)), dma((n2,)), pltpu.SemaphoreType.REGULAR,
        ],
        compiler_params=pltpu.CompilerParams(collective_id=0, has_side_effects=True, vmem_limit_bytes=67043328),
        cost_estimate=pl.CostEstimate(flops=6 * g_loc * rows * d * ff, bytes_accessed=6 * g_loc * d * ff, transcendentals=0),
        name="moe",
    )(meta, z, h, w1, w3, w2)


def solution(mesh):
    ep = mesh.shape['ep']
    tok = P(('dp', 'ep'))
    rep = P()
    exs = P('ep')

    def body(x, idx, gates, g1, wq, wk, wv, wo, g2, w1, w3, w2):
        n, s_len, d = x.shape
        t = n * s_len
        top = idx.shape[-1]
        avg = top * t // (w1.shape[0] * ep)
        cap = avg + avg // 2
        h, z, meta = attention(x.reshape(t, d), idx.transpose(0, 2, 1), gates.transpose(0, 2, 1), g1, g2, wq, wk, wv, wo, s_len, NZ, HB)
        return moe(ep, meta, z, h, w1, w3, w2, cap, NCOL).reshape(n, s_len, d)

    return jax.shard_map(body, mesh=mesh, in_specs=(tok, tok, tok, rep, rep, rep, rep, rep, rep, exs, exs, exs), out_specs=tok, check_vma=False)
```

```python
import functools

import jax
import jax.numpy as jnp
from jax import lax
from jax.experimental import pallas as pl
from jax.experimental.pallas import tpu as pltpu
from jax.sharding import PartitionSpec as P

EPS = 1e-6
HEAD = 128
F32, BF16 = jnp.float32, jnp.bfloat16


def rms(xf, g):
    return (xf * lax.rsqrt(jnp.mean(xf * xf, axis=-1, keepdims=True) + EPS) * g).astype(BF16)


def split3(g):
    hi = g.astype(BF16)
    r = g - hi.astype(F32)
    mid = r.astype(BF16)
    return hi, mid, (r - mid.astype(F32)).astype(BF16)


MESH = pl.DeviceIdType.MESH
NZ, NW, NW2, NCOL, HB = 8, 6, 8, 256, 4


def layer_kernel(ep, cfg, x_ref, idx_hbm, gate_hbm, g1_hbm, g2_hbm, wq_ref, wk_ref, wv_ref, wo_ref, w1_ref, w3_ref, w2_ref, y_ref,
                 idx_ref, gate_ref, g1_ref, g2_ref, mbuf, zbuf, dbuf, gbuf, wbuf, acc1, acc3, rbuf, ubuf, w2buf, h1buf, h2buf, h_ref,
                 load_sem, m_send, m_recv, z_send, z_recv, w_sem, w2_sem, r_send, r_recv, y_sem, ready):
    g_loc, cp, ncol = cfg
    nz, _, t, kc = zbuf.shape
    tp = mbuf.shape[2]
    ff = acc1.shape[2]
    d = nz * kc
    kw = 2 * kc
    nk = nz // 2
    rows = ep * cp
    chips = ep // 2
    half = t // 2
    n2 = d // ncol
    nq = ff // ncol
    fit = (rows - t) // cp
    hbw = HB * HEAD
    blocks = wq_ref.shape[1] // hbw
    assert d == 2 * ff and hbw == kw and ff == 2 * kw
    assert fit * nq >= ep
    nw, nw2 = wbuf.shape[0], w2buf.shape[0]

    me = lax.axis_index('ep')
    chip, core = me // 2, lax.rem(me, 2)
    rchip, lchip, ochip = lax.rem(chip + 1, chips), lax.rem(chip + chips - 1, chips), lax.rem(chip + 2, chips)
    right, left, opp, sib = rchip * 2 + core, lchip * 2 + core, ochip * 2 + core, chip * 2 + 1 - core

    def send(src, dst, ssem, rsem, dev):
        return pltpu.make_async_remote_copy(src_ref=src, dst_ref=dst, send_sem=ssem, recv_sem=rsem,
                                            device_id={'ep': dev}, device_id_type=MESH)

    def wcopy(n, which, unit):
        e, c = lax.rem(n, g_loc), n // g_loc
        ref = w3_ref if which else w1_ref
        slot = lax.rem(n + 4 * blocks, nw)
        row = pl.multiple_of((jnp.maximum(2 * c - 1, 0) + unit) * kc, kc)
        return pltpu.make_async_copy(ref.at[e, pl.ds(row, kc)], wbuf.at[slot, which, unit * kc:(unit + 1) * kc],
                                     w_sem.at[slot, which, unit])

    def wstart(n):
        @pl.when(n < (nk + 1) * g_loc)
        def _():
            wcopy(n, 0, 0).start()
            wcopy(n, 1, 0).start()

        @pl.when((n >= g_loc) & (n < nk * g_loc))
        def _():
            wcopy(n, 0, 1).start()
            wcopy(n, 1, 1).start()

    def w2copy(n):
        e, c = lax.rem(n, g_loc), n // g_loc
        slot = lax.rem(n, nw2)
        return pltpu.make_async_copy(w2_ref.at[e, :, pl.ds(pl.multiple_of(c * ncol, ncol), ncol)], w2buf.at[slot], w2_sem.at[slot])

    loads = [pltpu.make_async_copy(src, dst, load_sem.at[k]) for k, (src, dst) in enumerate((
        (idx_hbm, idx_ref), (gate_hbm, gate_ref), (x_ref, h_ref), (g1_hbm, g1_ref), (g2_hbm, g2_ref)))]

    def acopies(l):
        b, which, slot = l // 4, l % 4, l % nw
        at = slice(b * hbw, (b + 1) * hbw)
        if which == 3:
            return [pltpu.make_async_copy(wo_ref.at[at, a * ff:(a + 1) * ff], wbuf.at[slot, a], w_sem.at[slot, a, 0]) for a in range(2)]
        ref = (wq_ref, wk_ref, wv_ref)[which]
        return [pltpu.make_async_copy(ref.at[j * kw:(j + 1) * kw, at], wbuf.at[slot, j // 2, :, j % 2 * hbw:(j % 2 + 1) * hbw],
                                      w_sem.at[slot, j // 2, j % 2]) for j in range(4)]

    def lstart(l):
        if l < 4 * blocks:
            for copy in acopies(l):
                copy.start()
        else:
            wstart(jnp.int32(l - 4 * blocks))

    def lwait(l):
        for copy in acopies(l):
            copy.wait()

    for copy in loads:
        copy.start()
    for l in range(nw):
        lstart(l)

    barrier = pltpu.get_barrier_semaphore()
    for k in range(1, ep):
        pl.semaphore_signal(barrier, inc=1, device_id={'ep': lax.rem(me + k, ep)}, device_id_type=MESH)

    def mcopy(k):
        return send(mbuf.at[me], mbuf.at[me], m_send.at[k - 1], m_recv.at[k - 1], lax.rem(me + k, ep))

    def zcopy(c, k):
        if k == 3:
            ref, dev = zbuf.at[c, left, pl.ds(0, half)], right
        elif k == 4:
            ref, dev = zbuf.at[c, right, pl.ds(half, half)], left
        else:
            who, dev = {0: (me, right), 1: (me, left), 2: (me, sib), 5: (left, sib), 6: (right, sib), 7: (opp, sib)}[k]
            ref = zbuf.at[c, who]
        return send(ref, ref, z_send.at[c, k], z_recv.at[c, k], dev)

    def own(c):
        for k in (0, 1, 2):
            zcopy(c, k).start()

    def stage1(c):
        zcopy(c, 0).wait_recv()
        zcopy(c, 3).start()
        zcopy(c, 5).start()
        zcopy(c, 1).wait_recv()
        zcopy(c, 4).start()
        zcopy(c, 6).start()

    def stage2(c):
        zcopy(c, 3).wait_recv()
        zcopy(c, 4).wait_recv()
        zcopy(c, 7).start()

    def stage3(c):
        for k in (2, 5, 6, 7):
            zcopy(c, k).wait_recv()

    def hop(m):
        @pl.when(m < nz)
        def _():
            stage1(m)

        @pl.when(m + 2 < nz)
        def _():
            own(m + 2)

    def share(m):
        @pl.when(m < nz)
        def _():
            stage2(m)

    loads[0].wait()
    loads[1].wait()
    seqs, top, seq = idx_ref.shape
    ids, gts = jnp.zeros((top, tp), F32), jnp.zeros((top, tp), F32)
    for n in range(seqs):
        at, to = lax.broadcasted_iota(jnp.int32, (seq, tp), 0), lax.broadcasted_iota(jnp.int32, (seq, tp), 1)
        move = jnp.where(at + n * seq == to, 1.0, 0.0).astype(BF16)
        ids += jnp.dot(idx_ref[n].astype(F32).astype(BF16), move, preferred_element_type=F32)
        hi, mid, lo = [jnp.dot(p, move, preferred_element_type=F32) for p in split3(gate_ref[n])]
        gts += hi + mid + lo
    mbuf[me, :top] = jnp.where(lax.broadcasted_iota(jnp.int32, (top, tp), 1) < t, ids, -1.0)
    mbuf[me, top:] = gts

    for k in (2, 3, 4):
        loads[k].wait()
    xn = rms(h_ref[...].astype(F32), g1_ref[...])
    for a in range(2):
        ubuf[a, :t] = xn[:, a * ff:(a + 1) * ff]
    pl.semaphore_wait(barrier, ep - 1)
    for k in range(1, ep):
        mcopy(k).start()

    row = lax.broadcasted_iota(jnp.int32, (t, t), 0)
    col = lax.broadcasted_iota(jnp.int32, (t, t), 1)
    mask = (row >= col) & (row // seq == col // seq)

    def project(l):
        slot = l % nw
        parts = [jnp.dot(ubuf[j // 2, :t, j % 2 * kw:(j % 2 + 1) * kw], wbuf[slot, j // 2, :, j % 2 * hbw:(j % 2 + 1) * hbw],
                         preferred_element_type=F32) for j in range(4)]
        return (parts[0] + parts[1] + parts[2] + parts[3]).astype(BF16)

    for b in range(blocks):
        for k in range(3):
            lwait(4 * b + k)
        q, k, v = [project(4 * b + i) for i in range(3)]
        for i in range(3):
            lstart(4 * b + i + nw)
        outs = []
        for j in range(HB):
            sl = slice(j * HEAD, (j + 1) * HEAD)
            s = lax.dot_general(q[:, sl], k[:, sl], (((1,), (1,)), ((), ())), preferred_element_type=F32) * HEAD ** -0.5
            s = jnp.where(mask, s, -1e30)
            e = jnp.exp(s - jnp.max(s, axis=-1, keepdims=True))
            p = (e / jnp.sum(e, axis=-1, keepdims=True)).astype(BF16)
            outs.append(jnp.dot(p, v[:, sl], preferred_element_type=F32).astype(BF16))
        o = jnp.concatenate(outs, axis=1)
        lwait(4 * b + 3)
        for a in range(2):
            part = jnp.dot(o, wbuf[(4 * b + 3) % nw, a], preferred_element_type=F32)
            acc1[a, :t] = part if b == 0 else acc1[a, :t] + part
        lstart(4 * b + 3 + nw)

    h = (h_ref[...].astype(F32) + jnp.concatenate([acc1[0, :t], acc1[1, :t]], axis=1).astype(BF16).astype(F32)).astype(BF16)
    h_ref[...] = h
    z = rms(h.astype(F32), g2_ref[...])
    for m in range(nz):
        zbuf[m, me] = z[:, m * kc:(m + 1) * kc]
    for n in range(nw2):
        w2copy(n).start()
    own(0)
    own(1)
    for k in range(1, ep):
        mcopy(k).wait_recv()

    base = (me * g_loc).astype(F32)

    def build(s):
        m = mbuf[s]
        top = m.shape[0] // 2
        ids, gt = m[:top], m[top:]
        masks, gates = [], []
        for e in range(g_loc):
            hit = ids == base + float(e)
            masks.append(jnp.max(jnp.where(hit, 1.0, 0.0), axis=0, keepdims=True))
            gates.append(jnp.sum(jnp.where(hit, gt, 0.0), axis=0, keepdims=True))
        mask, gate = jnp.concatenate(masks, axis=0), jnp.concatenate(gates, axis=0)
        before = lax.broadcasted_iota(jnp.int32, (tp, tp), 0) < lax.broadcasted_iota(jnp.int32, (tp, tp), 1)
        rank = jnp.dot(mask.astype(BF16), jnp.where(before, 1.0, 0.0).astype(BF16), preferred_element_type=F32)
        place = jnp.where(mask > 0.5, rank, -1.0)
        slot = lax.broadcasted_iota(jnp.int32, (cp, t), 0).astype(F32)
        dbuf[s] = jnp.concatenate([jnp.where(slot == place[e:e + 1, :t], 1.0, 0.0) for e in range(g_loc)], axis=0).astype(BF16)
        re = lax.broadcasted_iota(jnp.int32, (g_loc, g_loc * cp), 0)
        rr = lax.broadcasted_iota(jnp.int32, (g_loc, g_loc * cp), 1)
        spread = jnp.where((rr >= re * cp) & (rr < re * cp + cp), 1.0, 0.0).astype(BF16)

        def widen(a):
            return lax.dot_general(a, spread, (((0,), (0,)), ((), ())), preferred_element_type=F32)[:t]

        slots = lax.rem(lax.broadcasted_iota(jnp.int32, (t, g_loc * cp), 1), cp).astype(F32)
        sel = widen(place.astype(BF16)) == slots
        for i, part in enumerate(split3(gate)):
            gbuf[s, i * t:(i + 1) * t] = jnp.where(sel, widen(part), 0.0).astype(BF16)

    def builds(i, _):
        for q in range(4):
            build(4 * i + q)
        hop(i)
        return 0

    lax.fori_loop(0, ep // 4, builds, 0)
    share(0)

    def dispatch(m, q):
        stage3(m)
        at = pl.ds(pl.multiple_of(q * kc, kc), kc)
        for p in range(ep // 2):
            a = jnp.dot(dbuf[2 * p], zbuf[m, 2 * p], preferred_element_type=F32)
            b = jnp.dot(dbuf[2 * p + 1], zbuf[m, 2 * p + 1], preferred_element_type=F32)
            for e in range(g_loc):
                sl = slice(e * cp, (e + 1) * cp)
                rbuf[e, p * 2 * cp:(p + 1) * 2 * cp, at] = jnp.concatenate([a[sl], b[sl]], axis=0).astype(BF16)

    def experts_in(c, kind):
        units = 2 if kind == 'mid' else 1
        k = units * kc

        def step(i, _):
            n = c * g_loc + 2 * i
            for q in range(2):
                for u in range(units):
                    wcopy(n + q, 0, u).wait()
                    wcopy(n + q, 1, u).wait()
            for q in range(2):
                e, slot = 2 * i + q, lax.rem(n + q + 4 * blocks, nw)
                r = rbuf[e, :, :k]
                a = jnp.dot(r, wbuf[slot, 0, :k], preferred_element_type=F32)
                b = jnp.dot(r, wbuf[slot, 1, :k], preferred_element_type=F32)
                if kind != 'first':
                    a = acc1[e] + a
                    b = acc3[e] + b
                if kind == 'last':
                    ubuf[e] = (a / (1.0 + jnp.exp(-a)) * b).astype(BF16)
                else:
                    acc1[e] = a
                    acc3[e] = b
            wstart(n + nw)
            wstart(n + nw + 1)
            return 0

        return step

    dispatch(0, 0)

    def opening(i, _):
        @pl.when(i > 0)
        def _():
            hop(2)
            share(1)

        return lax.fori_loop(i * 2, i * 2 + 2, experts_in(0, 'first'), 0)

    lax.fori_loop(0, g_loc // 4, opening, 0)
    hop(3)
    share(2)

    def chunk(c, _):
        def pick(q, _):
            dispatch(2 * c - 1 + q, q)
            return 0

        lax.fori_loop(0, 2, pick, 0)
        step = experts_in(c, 'mid')

        def portion(i, _):
            @pl.when(i > 0)
            def _():
                hop(2 * c + 1 + i)
                share(2 * c + i)

            return lax.fori_loop(i * 2 - jnp.minimum(i, 1), jnp.minimum(i * 2 + 1, g_loc // 2), step, 0)

        lax.fori_loop(0, 3, portion, 0)
        return 0

    lax.fori_loop(1, nk, chunk, 0)
    dispatch(nz - 1, 0)
    lax.fori_loop(0, g_loc // 2, experts_in(nk, 'last'), 0)
    pl.semaphore_signal(ready, inc=1, device_id={'ep': sib}, device_id_type=MESH)

    def cols(c):
        return pl.ds(pl.multiple_of(lax.rem(c, nq) * ncol, ncol), ncol)

    def rcopy(c, k):
        if k == 0:
            src = acc1.at[pl.ds(chips, chips), pl.ds(0, t), cols(c)]
            dst, dev = acc3.at[pl.ds(c // nq * chips, chips), pl.ds(0, t), cols(c)], sib
        elif k == 1:
            src, dst, dev = acc1.at[ochip, pl.ds(0, half), cols(c)], h1buf.at[c, 0], right
        elif k == 2:
            src, dst, dev = acc1.at[ochip, pl.ds(half, half), cols(c)], h1buf.at[c, 1], left
        elif k == 3:
            src, dst, dev = acc1.at[rchip, pl.ds(0, t), cols(c)], h2buf.at[c, 0], right
        else:
            src, dst, dev = acc1.at[lchip, pl.ds(0, t), cols(c)], h2buf.at[c, 1], left
        return send(src, dst, r_send.at[c, k], r_recv.at[c, k], dev)

    def out_cols(c):
        def step(i, _):
            n = c * g_loc + 4 * i
            for q in range(4):
                w2copy(n + q).wait()
            for q in range(4):
                e = 4 * i + q
                o = jnp.dot(ubuf[e], w2buf[lax.rem(n + q, nw2)], preferred_element_type=F32)
                o = o.astype(BF16).astype(F32)
                for r in range(ep):
                    acc3[e, t + r % fit * cp:t + (r % fit + 1) * cp, r // fit * ncol:(r // fit + 1) * ncol] = o[r * cp:(r + 1) * cp]

            @pl.when(n + nw2 < n2 * g_loc)
            def _():
                for q in range(4):
                    w2copy(n + q + nw2).start()

            return 0

        lax.fori_loop(0, g_loc // 4, step, 0)

        def comb(i, _):
            for q in range(4):
                s = 4 * i + q
                at = pl.ds(pl.multiple_of(t + lax.rem(s, fit) * cp, 8), cp), pl.ds(pl.multiple_of(s // fit * ncol, ncol), ncol)
                es = jnp.concatenate([acc3[e, at[0], at[1]] for e in range(g_loc)], axis=0).astype(BF16)
                p = jnp.dot(gbuf[s], es, preferred_element_type=F32)
                place = s // 2 + jnp.where(q % 2 == core, 0, chips)
                acc1[place, pl.ds(0, t), cols(c)] = p[:t] + p[t:2 * t] + p[2 * t:]
            return 0

        lax.fori_loop(0, ep // 4, comb, 0)

    def stage_b(c):
        rcopy(c, 0).wait_recv()

        def add(j, _):
            acc1[j, pl.ds(0, t), cols(c)] += acc3[c // nq * chips + j, pl.ds(0, t), cols(c)]
            return 0

        lax.fori_loop(0, chips, add, 0)
        rcopy(c, 1).start()
        rcopy(c, 2).start()

    def stage_c(c):
        rcopy(c, 1).wait_recv()
        acc1[rchip, pl.ds(0, half), cols(c)] += h1buf[c, 0]
        rcopy(c, 3).start()
        rcopy(c, 2).wait_recv()
        acc1[lchip, pl.ds(half, half), cols(c)] += h1buf[c, 1]
        rcopy(c, 4).start()

    def ycopy(c):
        at = pl.ds(pl.multiple_of(c * ncol, ncol), ncol)
        return pltpu.make_async_copy(h_ref.at[:, at], y_ref.at[:, at], y_sem.at[c])

    def stage_d(c):
        rcopy(c, 3).wait_recv()
        rcopy(c, 4).wait_recv()
        moe = acc1[chip, pl.ds(0, t), cols(c)] + h2buf[c, 0] + h2buf[c, 1]
        at = pl.ds(pl.multiple_of(c * ncol, ncol), ncol)
        h_ref[:, at] = (h_ref[:, at].astype(F32) + moe).astype(BF16)
        ycopy(c).start()
        for k in range(5):
            rcopy(c, k).wait_send()

    def tail_step(i, _):
        @pl.when(i < n2)
        def _():
            out_cols(i)

            @pl.when(i == 0)
            def _():
                pl.semaphore_wait(ready, 1)

            rcopy(i, 0).start()

        @pl.when((i >= 1) & (i - 1 < n2))
        def _():
            stage_b(i - 1)

        @pl.when((i >= 2) & (i - 2 < n2))
        def _():
            stage_c(i - 2)

        @pl.when(i >= 3)
        def _():
            stage_d(i - 3)

        return 0

    lax.fori_loop(0, n2 + 3, tail_step, 0)
    for k in range(1, ep):
        mcopy(k).wait_send()

    def drain(c, _):
        for k in range(8):
            zcopy(c, k).wait_send()
        return 0

    lax.fori_loop(0, nz, drain, 0)

    def finish(c, _):
        ycopy(c).wait()
        return 0

    lax.fori_loop(0, n2, finish, 0)


def layer(ep, x, idx, gates, g1, g2, wq, wk, wv, wo, w1, w3, w2, cap, ncol):
    t, d = x.shape
    g_loc, _, ff = w1.shape
    nz, kc, tp, top = NZ, d // NZ, t + -t % 128, idx.shape[1]
    cp = -(-cap // 8) * 8
    rows = ep * cp
    n2 = d // ncol
    vm = lambda *s: pltpu.VMEM(s, BF16)
    vf = lambda *s: pltpu.VMEM(s, F32)
    hbm = pl.BlockSpec(memory_space=pltpu.HBM)
    dma = pltpu.SemaphoreType.DMA
    return pl.pallas_call(
        functools.partial(layer_kernel, ep, (g_loc, cp, ncol)),
        in_specs=[hbm] * 12,
        out_specs=hbm,
        out_shape=jax.ShapeDtypeStruct((t, d), BF16),
        scratch_shapes=[
            pltpu.VMEM(idx.shape, jnp.int32), vf(*gates.shape), vf(1, d), vf(1, d), vf(ep, 2 * top, tp), vm(nz, ep, t, kc), vm(ep, g_loc * cp, t), vm(ep, 3 * t, g_loc * cp),
            vm(NW, 2, 2 * kc, ff), vf(g_loc, rows, ff), vf(g_loc, rows, ff), vm(g_loc, rows, 2 * kc), vm(g_loc, rows, ff),
            vm(NW2, ff, ncol), vf(n2, 2, t // 2, ncol), vf(n2, 2, t, ncol), vm(t, d),
            dma((5,)), dma((ep - 1,)), dma((ep - 1,)), dma((nz, 8)), dma((nz, 8)), dma((NW, 2, 2)), dma((NW2,)),
            dma((n2, 5)), dma((n2, 5)), dma((n2,)), pltpu.SemaphoreType.REGULAR,
        ],
        compiler_params=pltpu.CompilerParams(collective_id=0, has_side_effects=True, vmem_limit_bytes=67043328),
        cost_estimate=pl.CostEstimate(flops=6 * g_loc * rows * d * ff, bytes_accessed=6 * g_loc * d * ff, transcendentals=0),
        name="layer",
    )(x, idx, gates, g1.reshape(1, d), g2.reshape(1, d), wq, wk, wv, wo, w1, w3, w2)


def solution(mesh):
    ep = mesh.shape['ep']
    tok = P(('dp', 'ep'))
    rep = P()
    exs = P('ep')

    def body(x, idx, gates, g1, wq, wk, wv, wo, g2, w1, w3, w2):
        n, s_len, d = x.shape
        t = n * s_len
        top = idx.shape[-1]
        avg = top * t // (w1.shape[0] * ep)
        cap = avg + avg // 2
        y = layer(ep, x.reshape(t, d), idx.transpose(0, 2, 1), gates.transpose(0, 2, 1), g1, g2, wq, wk, wv, wo, w1, w3, w2, cap, NCOL)
        return y.reshape(n, s_len, d)

    return jax.shard_map(body, mesh=mesh, in_specs=(tok, tok, tok, rep, rep, rep, rep, rep, rep, exs, exs, exs), out_specs=tok, check_vma=False)
```

```python
import functools

import jax
import jax.numpy as jnp
from jax import lax
from jax.experimental import pallas as pl
from jax.experimental.pallas import tpu as pltpu
from jax.sharding import PartitionSpec as P

EPS = 1e-6
HEAD = 128
F32, BF16 = jnp.float32, jnp.bfloat16


def rms(xf, g):
    return (xf * lax.rsqrt(jnp.mean(xf * xf, axis=-1, keepdims=True) + EPS) * g).astype(BF16)


def split3(g):
    hi = g.astype(BF16)
    r = g - hi.astype(F32)
    mid = r.astype(BF16)
    return hi, mid, (r - mid.astype(F32)).astype(BF16)


MESH = pl.DeviceIdType.MESH
NZ, NW, NW2, NCOL, HB = 8, 6, 8, 256, 4


def layer_kernel(ep, cfg, x_ref, idx_hbm, gate_hbm, g1_hbm, g2_hbm, wq_ref, wk_ref, wv_ref, wo_ref, w1_ref, w3_ref, w2_ref, y_ref,
                 idx_ref, gate_ref, g1_ref, g2_ref, mbuf, zbuf, dbuf, gbuf, wbuf, acc1, acc3, rbuf, ubuf, w2buf, h1buf, h2buf, h_ref,
                 load_sem, m_send, m_recv, z_send, z_recv, w_sem, w2_sem, r_send, r_recv, y_sem, ready):
    g_loc, cp, ncol = cfg
    nz, _, t, kc = zbuf.shape
    tp = mbuf.shape[2]
    ff = acc1.shape[2]
    d = nz * kc
    kw = 2 * kc
    nk = nz // 2
    rows = ep * cp
    chips = ep // 2
    half = t // 2
    n2 = d // ncol
    nq = ff // ncol
    fit = (rows - t) // cp
    hbw = HB * HEAD
    blocks = wq_ref.shape[1] // hbw
    assert d == 2 * ff and hbw == kw and ff == 2 * kw
    assert fit * nq >= ep
    nw, nw2 = wbuf.shape[0], w2buf.shape[0]

    me = lax.axis_index('ep')
    chip, core = me // 2, lax.rem(me, 2)
    rchip, lchip, ochip = lax.rem(chip + 1, chips), lax.rem(chip + chips - 1, chips), lax.rem(chip + 2, chips)
    right, left, opp, sib = rchip * 2 + core, lchip * 2 + core, ochip * 2 + core, chip * 2 + 1 - core

    def send(src, dst, ssem, rsem, dev):
        return pltpu.make_async_remote_copy(src_ref=src, dst_ref=dst, send_sem=ssem, recv_sem=rsem,
                                            device_id={'ep': dev}, device_id_type=MESH)

    def wcopy(n, which, unit):
        e, c = lax.rem(n, g_loc), n // g_loc
        ref = w3_ref if which else w1_ref
        slot = lax.rem(n + 4 * blocks, nw)
        row = pl.multiple_of((jnp.maximum(2 * c - 1, 0) + unit) * kc, kc)
        return pltpu.make_async_copy(ref.at[e, pl.ds(row, kc)], wbuf.at[slot, which, unit * kc:(unit + 1) * kc],
                                     w_sem.at[slot, which, unit])

    def wstart(n):
        @pl.when(n < (nk + 1) * g_loc)
        def _():
            wcopy(n, 0, 0).start()
            wcopy(n, 1, 0).start()

        @pl.when((n >= g_loc) & (n < nk * g_loc))
        def _():
            wcopy(n, 0, 1).start()
            wcopy(n, 1, 1).start()

    def w2copy(n):
        e, c = lax.rem(n, g_loc), n // g_loc
        slot = lax.rem(n, nw2)
        return pltpu.make_async_copy(w2_ref.at[e, :, pl.ds(pl.multiple_of(c * ncol, ncol), ncol)], w2buf.at[slot], w2_sem.at[slot])

    loads = [pltpu.make_async_copy(src, dst, load_sem.at[k]) for k, (src, dst) in enumerate((
        (idx_hbm, idx_ref), (gate_hbm, gate_ref), (x_ref, h_ref), (g1_hbm, g1_ref), (g2_hbm, g2_ref)))]

    def acopies(l):
        b, which, slot = l // 4, l % 4, l % nw
        at = slice(b * hbw, (b + 1) * hbw)
        if which == 3:
            return [pltpu.make_async_copy(wo_ref.at[at, a * ff:(a + 1) * ff], wbuf.at[slot, a], w_sem.at[slot, a, 0]) for a in range(2)]
        ref = (wq_ref, wk_ref, wv_ref)[which]
        return [pltpu.make_async_copy(ref.at[j * kw:(j + 1) * kw, at], wbuf.at[slot, j // 2, :, j % 2 * hbw:(j % 2 + 1) * hbw],
                                      w_sem.at[slot, j // 2, j % 2]) for j in range(4)]

    def lstart(l):
        if l < 4 * blocks:
            for copy in acopies(l):
                copy.start()
        else:
            wstart(jnp.int32(l - 4 * blocks))

    def lwait(l):
        for copy in acopies(l):
            copy.wait()

    for copy in loads:
        copy.start()
    for l in range(nw):
        lstart(l)

    barrier = pltpu.get_barrier_semaphore()
    for k in range(1, ep):
        pl.semaphore_signal(barrier, inc=1, device_id={'ep': lax.rem(me + k, ep)}, device_id_type=MESH)

    def mcopy(k):
        return send(mbuf.at[me], mbuf.at[me], m_send.at[k - 1], m_recv.at[k - 1], lax.rem(me + k, ep))

    def zcopy(c, k):
        if k == 3:
            ref, dev = zbuf.at[c, left, pl.ds(0, half)], right
        elif k == 4:
            ref, dev = zbuf.at[c, right, pl.ds(half, half)], left
        else:
            who, dev = {0: (me, right), 1: (me, left), 2: (me, sib), 5: (left, sib), 6: (right, sib), 7: (opp, sib)}[k]
            ref = zbuf.at[c, who]
        return send(ref, ref, z_send.at[c, k], z_recv.at[c, k], dev)

    def own(c):
        for k in (0, 1, 2):
            zcopy(c, k).start()

    def stage1(c):
        zcopy(c, 0).wait_recv()
        zcopy(c, 3).start()
        zcopy(c, 5).start()
        zcopy(c, 1).wait_recv()
        zcopy(c, 4).start()
        zcopy(c, 6).start()

    def stage2(c):
        zcopy(c, 3).wait_recv()
        zcopy(c, 4).wait_recv()
        zcopy(c, 7).start()

    def stage3(c):
        for k in (2, 5, 6, 7):
            zcopy(c, k).wait_recv()

    def hop(m):
        @pl.when(m < nz)
        def _():
            stage1(m)

        @pl.when(m + 2 < nz)
        def _():
            own(m + 2)

    def share(m):
        @pl.when(m < nz)
        def _():
            stage2(m)

    loads[0].wait()
    loads[1].wait()
    seqs, top, seq = idx_ref.shape
    ids, gts = jnp.zeros((top, tp), F32), jnp.zeros((top, tp), F32)
    for n in range(seqs):
        at, to = lax.broadcasted_iota(jnp.int32, (seq, tp), 0), lax.broadcasted_iota(jnp.int32, (seq, tp), 1)
        move = jnp.where(at + n * seq == to, 1.0, 0.0).astype(BF16)
        ids += jnp.dot(idx_ref[n].astype(F32).astype(BF16), move, preferred_element_type=F32)
        hi, mid, lo = [jnp.dot(p, move, preferred_element_type=F32) for p in split3(gate_ref[n])]
        gts += hi + mid + lo
    mbuf[me, :top] = jnp.where(lax.broadcasted_iota(jnp.int32, (top, tp), 1) < t, ids, -1.0)
    mbuf[me, top:] = gts

    for k in (2, 3, 4):
        loads[k].wait()
    xn = rms(h_ref[...].astype(F32), g1_ref[...])
    for a in range(2):
        ubuf[a, :t] = xn[:, a * ff:(a + 1) * ff]
    pl.semaphore_wait(barrier, ep - 1)
    for k in range(1, ep):
        mcopy(k).start()

    row = lax.broadcasted_iota(jnp.int32, (t, t), 0)
    col = lax.broadcasted_iota(jnp.int32, (t, t), 1)
    mask = (row >= col) & (row // seq == col // seq)

    def project(l):
        slot = l % nw
        parts = [jnp.dot(ubuf[j // 2, :t, j % 2 * kw:(j % 2 + 1) * kw], wbuf[slot, j // 2, :, j % 2 * hbw:(j % 2 + 1) * hbw],
                         preferred_element_type=F32) for j in range(4)]
        return (parts[0] + parts[1] + parts[2] + parts[3]).astype(BF16)

    for b in range(blocks):
        for k in range(3):
            lwait(4 * b + k)
        q, k, v = [project(4 * b + i) for i in range(3)]
        for i in range(3):
            lstart(4 * b + i + nw)
        outs = []
        for j in range(HB):
            sl = slice(j * HEAD, (j + 1) * HEAD)
            s = lax.dot_general(q[:, sl], k[:, sl], (((1,), (1,)), ((), ())), preferred_element_type=F32) * HEAD ** -0.5
            s = jnp.where(mask, s, -1e30)
            e = jnp.exp(s - jnp.max(s, axis=-1, keepdims=True))
            p = (e / jnp.sum(e, axis=-1, keepdims=True)).astype(BF16)
            outs.append(jnp.dot(p, v[:, sl], preferred_element_type=F32).astype(BF16))
        o = jnp.concatenate(outs, axis=1)
        lwait(4 * b + 3)
        for a in range(2):
            part = jnp.dot(o, wbuf[(4 * b + 3) % nw, a], preferred_element_type=F32)
            acc1[a, :t] = part if b == 0 else acc1[a, :t] + part
        lstart(4 * b + 3 + nw)

    h = (h_ref[...].astype(F32) + jnp.concatenate([acc1[0, :t], acc1[1, :t]], axis=1).astype(BF16).astype(F32)).astype(BF16)
    h_ref[...] = h
    z = rms(h.astype(F32), g2_ref[...])
    for m in range(nz):
        zbuf[m, me] = z[:, m * kc:(m + 1) * kc]
    for n in range(nw2):
        w2copy(n).start()
    own(0)
    own(1)
    for k in range(1, ep):
        mcopy(k).wait_recv()

    base = (me * g_loc).astype(F32)

    def build(s):
        m = mbuf[s]
        top = m.shape[0] // 2
        ids, gt = m[:top], m[top:]
        masks, gates = [], []
        for e in range(g_loc):
            hit = ids == base + float(e)
            masks.append(jnp.max(jnp.where(hit, 1.0, 0.0), axis=0, keepdims=True))
            gates.append(jnp.sum(jnp.where(hit, gt, 0.0), axis=0, keepdims=True))
        mask, gate = jnp.concatenate(masks, axis=0), jnp.concatenate(gates, axis=0)
        before = lax.broadcasted_iota(jnp.int32, (tp, tp), 0) < lax.broadcasted_iota(jnp.int32, (tp, tp), 1)
        rank = jnp.dot(mask.astype(BF16), jnp.where(before, 1.0, 0.0).astype(BF16), preferred_element_type=F32)
        place = jnp.where(mask > 0.5, rank, -1.0)
        slot = lax.broadcasted_iota(jnp.int32, (cp, t), 0).astype(F32)
        dbuf[s] = jnp.concatenate([jnp.where(slot == place[e:e + 1, :t], 1.0, 0.0) for e in range(g_loc)], axis=0).astype(BF16)
        re = lax.broadcasted_iota(jnp.int32, (g_loc, g_loc * cp), 0)
        rr = lax.broadcasted_iota(jnp.int32, (g_loc, g_loc * cp), 1)
        spread = jnp.where((rr >= re * cp) & (rr < re * cp + cp), 1.0, 0.0).astype(BF16)

        def widen(a):
            return lax.dot_general(a, spread, (((0,), (0,)), ((), ())), preferred_element_type=F32)[:t]

        slots = lax.rem(lax.broadcasted_iota(jnp.int32, (t, g_loc * cp), 1), cp).astype(F32)
        sel = widen(place.astype(BF16)) == slots
        for i, part in enumerate(split3(gate)):
            gbuf[s, i * t:(i + 1) * t] = jnp.where(sel, widen(part), 0.0).astype(BF16)

    def builds(i, _):
        for q in range(4):
            build(4 * i + q)
        hop(i)
        return 0

    lax.fori_loop(0, ep // 4, builds, 0)
    share(0)

    def dispatch(m, q):
        stage3(m)
        at = pl.ds(pl.multiple_of(q * kc, kc), kc)
        for p in range(ep // 2):
            a = jnp.dot(dbuf[2 * p], zbuf[m, 2 * p], preferred_element_type=F32)
            b = jnp.dot(dbuf[2 * p + 1], zbuf[m, 2 * p + 1], preferred_element_type=F32)
            for e in range(g_loc):
                sl = slice(e * cp, (e + 1) * cp)
                rbuf[e, p * 2 * cp:(p + 1) * 2 * cp, at] = jnp.concatenate([a[sl], b[sl]], axis=0).astype(BF16)

    def experts_in(c, kind):
        units = 2 if kind == 'mid' else 1
        k = units * kc
        width = kc if kind == 'last' else ff

        def step(i, _):
            n = c * g_loc + 2 * i
            for q in range(2):
                for u in range(units):
                    wcopy(n + q, 0, u).wait()
                    wcopy(n + q, 1, u).wait()
            for q in range(2):
                e, slot = 2 * i + q, lax.rem(n + q + 4 * blocks, nw)
                r = rbuf[e, :, :k]
                for f in range(0, ff, width):
                    at = slice(f, f + width)
                    a = jnp.dot(r, wbuf[slot, 0, :k, at], preferred_element_type=F32)
                    b = jnp.dot(r, wbuf[slot, 1, :k, at], preferred_element_type=F32)
                    if kind != 'first':
                        a = acc1[e, :, at] + a
                        b = acc3[e, :, at] + b
                    if kind == 'last':
                        ubuf[e, :, at] = (a / (1.0 + jnp.exp(-a)) * b).astype(BF16)
                    else:
                        acc1[e, :, at] = a
                        acc3[e, :, at] = b
            wstart(n + nw)
            wstart(n + nw + 1)
            return 0

        return step

    dispatch(0, 0)

    def opening(i, _):
        @pl.when(i > 0)
        def _():
            hop(2)
            share(1)

        return lax.fori_loop(i * 2, i * 2 + 2, experts_in(0, 'first'), 0)

    lax.fori_loop(0, g_loc // 4, opening, 0)
    hop(3)
    share(2)

    def chunk(c, _):
        def pick(q, _):
            dispatch(2 * c - 1 + q, q)
            return 0

        lax.fori_loop(0, 2, pick, 0)
        step = experts_in(c, 'mid')

        def portion(i, _):
            @pl.when(i > 0)
            def _():
                hop(2 * c + 1 + i)
                share(2 * c + i)

            return lax.fori_loop(i * 2 - jnp.minimum(i, 1), jnp.minimum(i * 2 + 1, g_loc // 2), step, 0)

        lax.fori_loop(0, 3, portion, 0)
        return 0

    lax.fori_loop(1, nk, chunk, 0)
    dispatch(nz - 1, 0)
    lax.fori_loop(0, g_loc // 2, experts_in(nk, 'last'), 0)
    pl.semaphore_signal(ready, inc=1, device_id={'ep': sib}, device_id_type=MESH)

    def cols(c):
        return pl.ds(pl.multiple_of(lax.rem(c, nq) * ncol, ncol), ncol)

    def rcopy(c, k):
        if k == 0:
            src = acc1.at[pl.ds(chips, chips), pl.ds(0, t), cols(c)]
            dst, dev = acc3.at[pl.ds(c // nq * chips, chips), pl.ds(0, t), cols(c)], sib
        elif k == 1:
            src, dst, dev = acc1.at[ochip, pl.ds(0, half), cols(c)], h1buf.at[c, 0], right
        elif k == 2:
            src, dst, dev = acc1.at[ochip, pl.ds(half, half), cols(c)], h1buf.at[c, 1], left
        elif k == 3:
            src, dst, dev = acc1.at[rchip, pl.ds(0, t), cols(c)], h2buf.at[c, 0], right
        else:
            src, dst, dev = acc1.at[lchip, pl.ds(0, t), cols(c)], h2buf.at[c, 1], left
        return send(src, dst, r_send.at[c, k], r_recv.at[c, k], dev)

    def out_cols(c):
        def step(i, _):
            n = c * g_loc + 4 * i
            for q in range(4):
                w2copy(n + q).wait()
            for q in range(4):
                e = 4 * i + q
                o = jnp.dot(ubuf[e], w2buf[lax.rem(n + q, nw2)], preferred_element_type=F32)
                o = o.astype(BF16).astype(F32)
                for r in range(ep):
                    acc3[e, t + r % fit * cp:t + (r % fit + 1) * cp, r // fit * ncol:(r // fit + 1) * ncol] = o[r * cp:(r + 1) * cp]

            @pl.when(n + nw2 < n2 * g_loc)
            def _():
                for q in range(4):
                    w2copy(n + q + nw2).start()

            return 0

        lax.fori_loop(0, g_loc // 4, step, 0)

    def combine(c):
        def comb(i, _):
            for q in range(4):
                s = 4 * i + q
                at = pl.ds(pl.multiple_of(t + lax.rem(s, fit) * cp, 8), cp), pl.ds(pl.multiple_of(s // fit * ncol, ncol), ncol)
                es = jnp.concatenate([acc3[e, at[0], at[1]] for e in range(g_loc)], axis=0).astype(BF16)
                p = jnp.dot(gbuf[s], es, preferred_element_type=F32)
                place = s // 2 + jnp.where(q % 2 == core, 0, chips)
                acc1[place, pl.ds(0, t), cols(c)] = p[:t] + p[t:2 * t] + p[2 * t:]
            return 0

        lax.fori_loop(0, ep // 4, comb, 0)

    def stage_b(c):
        rcopy(c, 0).wait_recv()

        def add(j, _):
            acc1[j, pl.ds(0, t), cols(c)] += acc3[c // nq * chips + j, pl.ds(0, t), cols(c)]
            return 0

        lax.fori_loop(0, chips, add, 0)
        rcopy(c, 1).start()
        rcopy(c, 2).start()

    def stage_c(c):
        rcopy(c, 1).wait_recv()
        acc1[rchip, pl.ds(0, half), cols(c)] += h1buf[c, 0]
        rcopy(c, 3).start()
        rcopy(c, 2).wait_recv()
        acc1[lchip, pl.ds(half, half), cols(c)] += h1buf[c, 1]
        rcopy(c, 4).start()

    def ycopy(c):
        at = pl.ds(pl.multiple_of(c * ncol, ncol), ncol)
        return pltpu.make_async_copy(h_ref.at[:, at], y_ref.at[:, at], y_sem.at[c])

    def stage_d(c):
        rcopy(c, 3).wait_recv()
        rcopy(c, 4).wait_recv()
        moe = acc1[chip, pl.ds(0, t), cols(c)] + h2buf[c, 0] + h2buf[c, 1]
        at = pl.ds(pl.multiple_of(c * ncol, ncol), ncol)
        h_ref[:, at] = (h_ref[:, at].astype(F32) + moe).astype(BF16)
        ycopy(c).start()
        for k in range(5):
            rcopy(c, k).wait_send()

    def tail_step(i, _):
        @pl.when(i < n2)
        def _():
            out_cols(i)

        @pl.when((i >= 1) & (i - 1 < n2))
        def _():
            stage_b(i - 1)

        @pl.when((i >= 2) & (i - 2 < n2))
        def _():
            stage_c(i - 2)

        @pl.when(i < n2)
        def _():
            combine(i)

            @pl.when(i == 0)
            def _():
                pl.semaphore_wait(ready, 1)

            rcopy(i, 0).start()

        @pl.when(i >= 3)
        def _():
            stage_d(i - 3)

        return 0

    lax.fori_loop(0, n2 + 3, tail_step, 0)
    for k in range(1, ep):
        mcopy(k).wait_send()

    def drain(c, _):
        for k in range(8):
            zcopy(c, k).wait_send()
        return 0

    lax.fori_loop(0, nz, drain, 0)

    def finish(c, _):
        ycopy(c).wait()
        return 0

    lax.fori_loop(0, n2, finish, 0)


def layer(ep, x, idx, gates, g1, g2, wq, wk, wv, wo, w1, w3, w2, cap, ncol):
    t, d = x.shape
    g_loc, _, ff = w1.shape
    nz, kc, tp, top = NZ, d // NZ, t + -t % 128, idx.shape[1]
    cp = -(-cap // 8) * 8
    rows = ep * cp
    n2 = d // ncol
    vm = lambda *s: pltpu.VMEM(s, BF16)
    vf = lambda *s: pltpu.VMEM(s, F32)
    hbm = pl.BlockSpec(memory_space=pltpu.HBM)
    dma = pltpu.SemaphoreType.DMA
    return pl.pallas_call(
        functools.partial(layer_kernel, ep, (g_loc, cp, ncol)),
        in_specs=[hbm] * 12,
        out_specs=hbm,
        out_shape=jax.ShapeDtypeStruct((t, d), BF16),
        scratch_shapes=[
            pltpu.VMEM(idx.shape, jnp.int32), vf(*gates.shape), vf(1, d), vf(1, d), vf(ep, 2 * top, tp), vm(nz, ep, t, kc), vm(ep, g_loc * cp, t), vm(ep, 3 * t, g_loc * cp),
            vm(NW, 2, 2 * kc, ff), vf(g_loc, rows, ff), vf(g_loc, rows, ff), vm(g_loc, rows, 2 * kc), vm(g_loc, rows, ff),
            vm(NW2, ff, ncol), vf(n2, 2, t // 2, ncol), vf(n2, 2, t, ncol), vm(t, d),
            dma((5,)), dma((ep - 1,)), dma((ep - 1,)), dma((nz, 8)), dma((nz, 8)), dma((NW, 2, 2)), dma((NW2,)),
            dma((n2, 5)), dma((n2, 5)), dma((n2,)), pltpu.SemaphoreType.REGULAR,
        ],
        compiler_params=pltpu.CompilerParams(collective_id=0, has_side_effects=True, vmem_limit_bytes=67043328),
        cost_estimate=pl.CostEstimate(flops=6 * g_loc * rows * d * ff, bytes_accessed=6 * g_loc * d * ff, transcendentals=0),
        name="layer",
    )(x, idx, gates, g1.reshape(1, d), g2.reshape(1, d), wq, wk, wv, wo, w1, w3, w2)


def solution(mesh):
    ep = mesh.shape['ep']
    tok = P(('dp', 'ep'))
    rep = P()
    exs = P('ep')

    def body(x, idx, gates, g1, wq, wk, wv, wo, g2, w1, w3, w2):
        n, s_len, d = x.shape
        t = n * s_len
        top = idx.shape[-1]
        avg = top * t // (w1.shape[0] * ep)
        cap = avg + avg // 2
        y = layer(ep, x.reshape(t, d), idx.transpose(0, 2, 1), gates.transpose(0, 2, 1), g1, g2, wq, wk, wv, wo, w1, w3, w2, cap, NCOL)
        return y.reshape(n, s_len, d)

    return jax.shard_map(body, mesh=mesh, in_specs=(tok, tok, tok, rep, rep, rep, rep, rep, rep, exs, exs, exs), out_specs=tok, check_vma=False)
```

```python
import functools

import jax
import jax.numpy as jnp
from jax import lax
from jax.experimental import pallas as pl
from jax.experimental.pallas import tpu as pltpu
from jax.sharding import PartitionSpec as P

EPS = 1e-6
HEAD = 128
F32, BF16 = jnp.float32, jnp.bfloat16


def rms(xf, g):
    return (xf * lax.rsqrt(jnp.mean(xf * xf, axis=-1, keepdims=True) + EPS) * g).astype(BF16)


def split3(g):
    hi = g.astype(BF16)
    r = g - hi.astype(F32)
    mid = r.astype(BF16)
    return hi, mid, (r - mid.astype(F32)).astype(BF16)


MESH = pl.DeviceIdType.MESH
NZ, NW, NW2, NCOL, HB = 8, 6, 8, 256, 4


def layer_kernel(ep, cfg, x_ref, idx_hbm, gate_hbm, g1_hbm, g2_hbm, wq_ref, wk_ref, wv_ref, wo_ref, w1_ref, w3_ref, w2_ref, y_ref,
                 idx_ref, gate_ref, g1_ref, g2_ref, mbuf, zbuf, dbuf, gbuf, wbuf, acc1, acc3, rbuf, ubuf, w2buf, h1buf, h2buf, h_ref,
                 load_sem, m_send, m_recv, z_send, z_recv, w_sem, w2_sem, r_send, r_recv, y_sem, ready):
    g_loc, cp, ncol = cfg
    nz, _, t, kc = zbuf.shape
    tp = mbuf.shape[2]
    ff = acc1.shape[2]
    d = nz * kc
    kw = 2 * kc
    nk = nz // 2
    rows = ep * cp
    chips = ep // 2
    half = t // 2
    n2 = d // ncol
    nq = ff // ncol
    fit = (rows - t) // cp
    hbw = HB * HEAD
    blocks = wq_ref.shape[1] // hbw
    assert d == 2 * ff and hbw == kw and ff == 2 * kw
    assert fit * nq >= ep
    nw, nw2 = wbuf.shape[0], w2buf.shape[0]

    me = lax.axis_index('ep')
    chip, core = me // 2, lax.rem(me, 2)
    rchip, lchip, ochip = lax.rem(chip + 1, chips), lax.rem(chip + chips - 1, chips), lax.rem(chip + 2, chips)
    right, left, opp, sib = rchip * 2 + core, lchip * 2 + core, ochip * 2 + core, chip * 2 + 1 - core

    def send(src, dst, ssem, rsem, dev):
        return pltpu.make_async_remote_copy(src_ref=src, dst_ref=dst, send_sem=ssem, recv_sem=rsem,
                                            device_id={'ep': dev}, device_id_type=MESH)

    def wcopy(n, which, unit):
        e, c = lax.rem(n, g_loc), n // g_loc
        ref = w3_ref if which else w1_ref
        slot = lax.rem(n + 4 * blocks, nw)
        row = pl.multiple_of((jnp.maximum(2 * c - 1, 0) + unit) * kc, kc)
        return pltpu.make_async_copy(ref.at[e, pl.ds(row, kc)], wbuf.at[slot, which, unit * kc:(unit + 1) * kc],
                                     w_sem.at[slot, which, unit])

    def wstart(n):
        @pl.when(n < (nk + 1) * g_loc)
        def _():
            wcopy(n, 0, 0).start()
            wcopy(n, 1, 0).start()

        @pl.when((n >= g_loc) & (n < nk * g_loc))
        def _():
            wcopy(n, 0, 1).start()
            wcopy(n, 1, 1).start()

    def w2copy(n):
        e, c = lax.rem(n, g_loc), n // g_loc
        slot = lax.rem(n, nw2)
        return pltpu.make_async_copy(w2_ref.at[e, :, pl.ds(pl.multiple_of(c * ncol, ncol), ncol)], w2buf.at[slot], w2_sem.at[slot])

    loads = [pltpu.make_async_copy(src, dst, load_sem.at[k]) for k, (src, dst) in enumerate((
        (idx_hbm, idx_ref), (gate_hbm, gate_ref), (x_ref, h_ref), (g1_hbm, g1_ref), (g2_hbm, g2_ref)))]

    def acopies(l):
        b, which, slot = l // 4, l % 4, l % nw
        at = slice(b * hbw, (b + 1) * hbw)
        if which == 3:
            return [pltpu.make_async_copy(wo_ref.at[at, a * ff:(a + 1) * ff], wbuf.at[slot, a], w_sem.at[slot, a, 0]) for a in range(2)]
        ref = (wq_ref, wk_ref, wv_ref)[which]
        return [pltpu.make_async_copy(ref.at[j * kw:(j + 1) * kw, at], wbuf.at[slot, j // 2, :, j % 2 * hbw:(j % 2 + 1) * hbw],
                                      w_sem.at[slot, j // 2, j % 2]) for j in range(4)]

    def lstart(l):
        if l < 4 * blocks:
            for copy in acopies(l):
                copy.start()
        else:
            wstart(jnp.int32(l - 4 * blocks))

    def lwait(l):
        for copy in acopies(l):
            copy.wait()

    for copy in loads:
        copy.start()
    for l in range(nw):
        lstart(l)

    barrier = pltpu.get_barrier_semaphore()
    for k in range(1, ep):
        pl.semaphore_signal(barrier, inc=1, device_id={'ep': lax.rem(me + k, ep)}, device_id_type=MESH)

    def mcopy(k):
        return send(mbuf.at[me], mbuf.at[me], m_send.at[k - 1], m_recv.at[k - 1], lax.rem(me + k, ep))

    def zcopy(c, k):
        if k == 3:
            ref, dev = zbuf.at[c, left, pl.ds(0, half)], right
        elif k == 4:
            ref, dev = zbuf.at[c, right, pl.ds(half, half)], left
        else:
            who, dev = {0: (me, right), 1: (me, left), 2: (me, sib), 5: (left, sib), 6: (right, sib), 7: (opp, sib)}[k]
            ref = zbuf.at[c, who]
        return send(ref, ref, z_send.at[c, k], z_recv.at[c, k], dev)

    def own(c):
        for k in (0, 1, 2):
            zcopy(c, k).start()

    def stage1(c):
        zcopy(c, 0).wait_recv()
        zcopy(c, 3).start()
        zcopy(c, 5).start()
        zcopy(c, 1).wait_recv()
        zcopy(c, 4).start()
        zcopy(c, 6).start()

    def stage2(c):
        zcopy(c, 3).wait_recv()
        zcopy(c, 4).wait_recv()
        zcopy(c, 7).start()

    def stage3(c):
        for k in (2, 5, 6, 7):
            zcopy(c, k).wait_recv()

    def hop(m):
        @pl.when(m < nz)
        def _():
            stage1(m)

        @pl.when(m + 2 < nz)
        def _():
            own(m + 2)

    def share(m):
        @pl.when(m < nz)
        def _():
            stage2(m)

    loads[0].wait()
    loads[1].wait()
    seqs, top, seq = idx_ref.shape
    ids, gts = jnp.zeros((top, tp), F32), jnp.zeros((top, tp), F32)
    for n in range(seqs):
        at, to = lax.broadcasted_iota(jnp.int32, (seq, tp), 0), lax.broadcasted_iota(jnp.int32, (seq, tp), 1)
        move = jnp.where(at + n * seq == to, 1.0, 0.0).astype(BF16)
        ids += jnp.dot(idx_ref[n].astype(F32).astype(BF16), move, preferred_element_type=F32)
        hi, mid, lo = [jnp.dot(p, move, preferred_element_type=F32) for p in split3(gate_ref[n])]
        gts += hi + mid + lo
    mbuf[me, :top] = jnp.where(lax.broadcasted_iota(jnp.int32, (top, tp), 1) < t, ids, -1.0)
    mbuf[me, top:] = gts

    for k in (2, 3, 4):
        loads[k].wait()
    xn = rms(h_ref[...].astype(F32), g1_ref[...])
    for a in range(2):
        ubuf[a, :t] = xn[:, a * ff:(a + 1) * ff]
    pl.semaphore_wait(barrier, ep - 1)
    for k in range(1, ep):
        mcopy(k).start()

    row = lax.broadcasted_iota(jnp.int32, (t, t), 0)
    col = lax.broadcasted_iota(jnp.int32, (t, t), 1)
    mask = (row >= col) & (row // seq == col // seq)

    def project(l):
        slot = l % nw
        parts = [jnp.dot(ubuf[j // 2, :t, j % 2 * kw:(j % 2 + 1) * kw], wbuf[slot, j // 2, :, j % 2 * hbw:(j % 2 + 1) * hbw],
                         preferred_element_type=F32) for j in range(4)]
        return (parts[0] + parts[1] + parts[2] + parts[3]).astype(BF16)

    for b in range(blocks):
        qkv = []
        for i in range(3):
            for l in range(4 * b, 4 * b + 3) if b and i == 0 else [4 * b + i] * (b == 0):
                lwait(l)
            qkv.append(project(4 * b + i))
        q, k, v = qkv
        for i in range(3):
            lstart(4 * b + i + nw)
        outs = []
        for j in range(HB):
            sl = slice(j * HEAD, (j + 1) * HEAD)
            s = lax.dot_general(q[:, sl], k[:, sl], (((1,), (1,)), ((), ())), preferred_element_type=F32) * HEAD ** -0.5
            s = jnp.where(mask, s, -1e30)
            e = jnp.exp(s - jnp.max(s, axis=-1, keepdims=True))
            p = (e / jnp.sum(e, axis=-1, keepdims=True)).astype(BF16)
            outs.append(jnp.dot(p, v[:, sl], preferred_element_type=F32).astype(BF16))
        o = jnp.concatenate(outs, axis=1)
        lwait(4 * b + 3)
        for a in range(2):
            part = jnp.dot(o, wbuf[(4 * b + 3) % nw, a], preferred_element_type=F32)
            acc1[a, :t] = part if b == 0 else acc1[a, :t] + part
        lstart(4 * b + 3 + nw)

    h = (h_ref[...].astype(F32) + jnp.concatenate([acc1[0, :t], acc1[1, :t]], axis=1).astype(BF16).astype(F32)).astype(BF16)
    h_ref[...] = h
    z = rms(h.astype(F32), g2_ref[...])
    for m in range(nz):
        zbuf[m, me] = z[:, m * kc:(m + 1) * kc]
    for n in range(nw2):
        w2copy(n).start()
    own(0)
    own(1)
    for k in range(1, ep):
        mcopy(k).wait_recv()

    base = (me * g_loc).astype(F32)

    def build(s):
        m = mbuf[s]
        top = m.shape[0] // 2
        ids, gt = m[:top], m[top:]
        masks, gates = [], []
        for e in range(g_loc):
            hit = ids == base + float(e)
            masks.append(jnp.max(jnp.where(hit, 1.0, 0.0), axis=0, keepdims=True))
            gates.append(jnp.sum(jnp.where(hit, gt, 0.0), axis=0, keepdims=True))
        mask, gate = jnp.concatenate(masks, axis=0), jnp.concatenate(gates, axis=0)
        before = lax.broadcasted_iota(jnp.int32, (tp, tp), 0) < lax.broadcasted_iota(jnp.int32, (tp, tp), 1)
        rank = jnp.dot(mask.astype(BF16), jnp.where(before, 1.0, 0.0).astype(BF16), preferred_element_type=F32)
        place = jnp.where(mask > 0.5, rank, -1.0)
        slot = lax.broadcasted_iota(jnp.int32, (cp, t), 0).astype(F32)
        dbuf[s] = jnp.concatenate([jnp.where(slot == place[e:e + 1, :t], 1.0, 0.0) for e in range(g_loc)], axis=0).astype(BF16)
        re = lax.broadcasted_iota(jnp.int32, (g_loc, g_loc * cp), 0)
        rr = lax.broadcasted_iota(jnp.int32, (g_loc, g_loc * cp), 1)
        spread = jnp.where((rr >= re * cp) & (rr < re * cp + cp), 1.0, 0.0).astype(BF16)

        def widen(a):
            return lax.dot_general(a, spread, (((0,), (0,)), ((), ())), preferred_element_type=F32)[:t]

        slots = lax.rem(lax.broadcasted_iota(jnp.int32, (t, g_loc * cp), 1), cp).astype(F32)
        sel = widen(place.astype(BF16)) == slots
        for i, part in enumerate(split3(gate)):
            gbuf[s, i * t:(i + 1) * t] = jnp.where(sel, widen(part), 0.0).astype(BF16)

    def builds(i, _):
        for q in range(4):
            build(4 * i + q)
        hop(i)
        return 0

    lax.fori_loop(0, ep // 4, builds, 0)
    share(0)

    def dispatch(m, q):
        stage3(m)
        at = pl.ds(pl.multiple_of(q * kc, kc), kc)
        for p in range(ep // 2):
            a = jnp.dot(dbuf[2 * p], zbuf[m, 2 * p], preferred_element_type=F32)
            b = jnp.dot(dbuf[2 * p + 1], zbuf[m, 2 * p + 1], preferred_element_type=F32)
            for e in range(g_loc):
                sl = slice(e * cp, (e + 1) * cp)
                rbuf[e, p * 2 * cp:(p + 1) * 2 * cp, at] = jnp.concatenate([a[sl], b[sl]], axis=0).astype(BF16)

    def experts_in(c, kind):
        units = 2 if kind == 'mid' else 1
        k = units * kc
        width = kc if kind == 'last' else ff

        def step(i, _):
            n = c * g_loc + 2 * i
            for q in range(2):
                for u in range(units):
                    wcopy(n + q, 0, u).wait()
                    wcopy(n + q, 1, u).wait()
            for q in range(2):
                e, slot = 2 * i + q, lax.rem(n + q + 4 * blocks, nw)
                r = rbuf[e, :, :k]
                for f in range(0, ff, width):
                    at = slice(f, f + width)
                    a = jnp.dot(r, wbuf[slot, 0, :k, at], preferred_element_type=F32)
                    b = jnp.dot(r, wbuf[slot, 1, :k, at], preferred_element_type=F32)
                    if kind != 'first':
                        a = acc1[e, :, at] + a
                        b = acc3[e, :, at] + b
                    if kind == 'last':
                        ubuf[e, :, at] = (a / (1.0 + jnp.exp(-a)) * b).astype(BF16)
                    else:
                        acc1[e, :, at] = a
                        acc3[e, :, at] = b
            wstart(n + nw)
            wstart(n + nw + 1)
            return 0

        return step

    dispatch(0, 0)

    def opening(i, _):
        @pl.when(i > 0)
        def _():
            hop(2)
            share(1)

        return lax.fori_loop(i * 2, i * 2 + 2, experts_in(0, 'first'), 0)

    lax.fori_loop(0, g_loc // 4, opening, 0)
    hop(3)
    share(2)

    def chunk(c, _):
        def pick(q, _):
            dispatch(2 * c - 1 + q, q)
            return 0

        lax.fori_loop(0, 2, pick, 0)
        step = experts_in(c, 'mid')

        def portion(i, _):
            @pl.when(i > 0)
            def _():
                hop(2 * c + 1 + i)
                share(2 * c + i)

            return lax.fori_loop(i * 2 - jnp.minimum(i, 1), jnp.minimum(i * 2 + 1, g_loc // 2), step, 0)

        lax.fori_loop(0, 3, portion, 0)
        return 0

    lax.fori_loop(1, nk, chunk, 0)
    dispatch(nz - 1, 0)
    lax.fori_loop(0, g_loc // 2, experts_in(nk, 'last'), 0)
    pl.semaphore_signal(ready, inc=1, device_id={'ep': sib}, device_id_type=MESH)

    def cols(c):
        return pl.ds(pl.multiple_of(lax.rem(c, nq) * ncol, ncol), ncol)

    def rcopy(c, k):
        if k == 0:
            src = acc1.at[pl.ds(chips, chips), pl.ds(0, t), cols(c)]
            dst, dev = acc3.at[pl.ds(c // nq * chips, chips), pl.ds(0, t), cols(c)], sib
        elif k == 1:
            src, dst, dev = acc1.at[ochip, pl.ds(0, half), cols(c)], h1buf.at[c, 0], right
        elif k == 2:
            src, dst, dev = acc1.at[ochip, pl.ds(half, half), cols(c)], h1buf.at[c, 1], left
        elif k == 3:
            src, dst, dev = acc1.at[rchip, pl.ds(0, t), cols(c)], h2buf.at[c, 0], right
        else:
            src, dst, dev = acc1.at[lchip, pl.ds(0, t), cols(c)], h2buf.at[c, 1], left
        return send(src, dst, r_send.at[c, k], r_recv.at[c, k], dev)

    def out_cols(c):
        def step(i, _):
            n = c * g_loc + 4 * i
            for q in range(4):
                w2copy(n + q).wait()
            for q in range(4):
                e = 4 * i + q
                o = jnp.dot(ubuf[e], w2buf[lax.rem(n + q, nw2)], preferred_element_type=F32)
                o = o.astype(BF16).astype(F32)
                for r in range(ep):
                    acc3[e, t + r % fit * cp:t + (r % fit + 1) * cp, r // fit * ncol:(r // fit + 1) * ncol] = o[r * cp:(r + 1) * cp]

            @pl.when(n + nw2 < n2 * g_loc)
            def _():
                for q in range(4):
                    w2copy(n + q + nw2).start()

            return 0

        lax.fori_loop(0, g_loc // 4, step, 0)

    def combine(c):
        def comb(i, _):
            for q in range(ep):
                s = jnp.int32(q)
                at = pl.ds(pl.multiple_of(t + lax.rem(s, fit) * cp, 8), cp), pl.ds(pl.multiple_of(s // fit * ncol, ncol), ncol)
                es = jnp.concatenate([acc3[e, at[0], at[1]] for e in range(g_loc)], axis=0).astype(BF16)
                p = jnp.dot(gbuf[s], es, preferred_element_type=F32)
                place = s // 2 + jnp.where(q % 2 == core, 0, chips)
                acc1[place, pl.ds(0, t), cols(c)] = p[:t] + p[t:2 * t] + p[2 * t:]
            return 0

        comb(0, 0)

    def stage_b(c):
        rcopy(c, 0).wait_recv()

        def add(j, _):
            acc1[j, pl.ds(0, t), cols(c)] += acc3[c // nq * chips + j, pl.ds(0, t), cols(c)]
            return 0

        lax.fori_loop(0, chips, add, 0)
        rcopy(c, 1).start()
        rcopy(c, 2).start()

    def stage_c(c):
        rcopy(c, 1).wait_recv()
        acc1[rchip, pl.ds(0, half), cols(c)] += h1buf[c, 0]
        rcopy(c, 3).start()
        rcopy(c, 2).wait_recv()
        acc1[lchip, pl.ds(half, half), cols(c)] += h1buf[c, 1]
        rcopy(c, 4).start()

    def ycopy(c):
        at = pl.ds(pl.multiple_of(c * ncol, ncol), ncol)
        return pltpu.make_async_copy(h_ref.at[:, at], y_ref.at[:, at], y_sem.at[c])

    def stage_d(c):
        rcopy(c, 3).wait_recv()
        rcopy(c, 4).wait_recv()
        moe = acc1[chip, pl.ds(0, t), cols(c)] + h2buf[c, 0] + h2buf[c, 1]
        at = pl.ds(pl.multiple_of(c * ncol, ncol), ncol)
        h_ref[:, at] = (h_ref[:, at].astype(F32) + moe).astype(BF16)
        ycopy(c).start()
        for k in range(5):
            rcopy(c, k).wait_send()

    def tail_step(i, _):
        @pl.when(i < n2)
        def _():
            out_cols(i)

        @pl.when((i >= 1) & (i - 1 < n2))
        def _():
            stage_b(i - 1)

        @pl.when((i >= 2) & (i - 2 < n2))
        def _():
            stage_c(i - 2)

        @pl.when(i < n2)
        def _():
            combine(i)

            @pl.when(i == 0)
            def _():
                pl.semaphore_wait(ready, 1)

            rcopy(i, 0).start()

        @pl.when(i >= 3)
        def _():
            stage_d(i - 3)

        return 0

    lax.fori_loop(0, n2 + 3, tail_step, 0)
    for k in range(1, ep):
        mcopy(k).wait_send()

    def drain(c, _):
        for k in range(8):
            zcopy(c, k).wait_send()
        return 0

    lax.fori_loop(0, nz, drain, 0)

    def finish(c, _):
        ycopy(c).wait()
        return 0

    lax.fori_loop(0, n2, finish, 0)


def layer(ep, x, idx, gates, g1, g2, wq, wk, wv, wo, w1, w3, w2, cap, ncol):
    t, d = x.shape
    g_loc, _, ff = w1.shape
    nz, kc, tp, top = NZ, d // NZ, t + -t % 128, idx.shape[1]
    cp = -(-cap // 8) * 8
    rows = ep * cp
    n2 = d // ncol
    vm = lambda *s: pltpu.VMEM(s, BF16)
    vf = lambda *s: pltpu.VMEM(s, F32)
    hbm = pl.BlockSpec(memory_space=pltpu.HBM)
    dma = pltpu.SemaphoreType.DMA
    return pl.pallas_call(
        functools.partial(layer_kernel, ep, (g_loc, cp, ncol)),
        in_specs=[hbm] * 12,
        out_specs=hbm,
        out_shape=jax.ShapeDtypeStruct((t, d), BF16),
        scratch_shapes=[
            pltpu.VMEM(idx.shape, jnp.int32), vf(*gates.shape), vf(1, d), vf(1, d), vf(ep, 2 * top, tp), vm(nz, ep, t, kc), vm(ep, g_loc * cp, t), vm(ep, 3 * t, g_loc * cp),
            vm(NW, 2, 2 * kc, ff), vf(g_loc, rows, ff), vf(g_loc, rows, ff), vm(g_loc, rows, 2 * kc), vm(g_loc, rows, ff),
            vm(NW2, ff, ncol), vf(n2, 2, t // 2, ncol), vf(n2, 2, t, ncol), vm(t, d),
            dma((5,)), dma((ep - 1,)), dma((ep - 1,)), dma((nz, 8)), dma((nz, 8)), dma((NW, 2, 2)), dma((NW2,)),
            dma((n2, 5)), dma((n2, 5)), dma((n2,)), pltpu.SemaphoreType.REGULAR,
        ],
        compiler_params=pltpu.CompilerParams(collective_id=0, has_side_effects=True, vmem_limit_bytes=67043328),
        cost_estimate=pl.CostEstimate(flops=6 * g_loc * rows * d * ff, bytes_accessed=6 * g_loc * d * ff, transcendentals=0),
        name="layer",
    )(x, idx, gates, g1.reshape(1, d), g2.reshape(1, d), wq, wk, wv, wo, w1, w3, w2)


def solution(mesh):
    ep = mesh.shape['ep']
    tok = P(('dp', 'ep'))
    rep = P()
    exs = P('ep')

    def body(x, idx, gates, g1, wq, wk, wv, wo, g2, w1, w3, w2):
        n, s_len, d = x.shape
        t = n * s_len
        top = idx.shape[-1]
        avg = top * t // (w1.shape[0] * ep)
        cap = avg + avg // 2
        y = layer(ep, x.reshape(t, d), idx.transpose(0, 2, 1), gates.transpose(0, 2, 1), g1, g2, wq, wk, wv, wo, w1, w3, w2, cap, NCOL)
        return y.reshape(n, s_len, d)

    return jax.shard_map(body, mesh=mesh, in_specs=(tok, tok, tok, rep, rep, rep, rep, rep, rep, exs, exs, exs), out_specs=tok, check_vma=False)
```
